32 devices in a mesh: dp: 1 (over z), ep: 32 (over y, x, core).
Axes of the slice: x: 4, y: 4, z: 1, core: 2. Of those that a mesh axis runs over, the one named last changes fastest.
The devices are a block of a 4x4x8 slice.
Arguments:
- grad_out: bfloat16 [2, 4096, 1536], P(None, ('dp', 'ep'))
- expert_out: bfloat16 [2, 4096, 6, 1536], P(None, ('dp', 'ep'))
- gate_vals: float32 [2, 4096, 6], P(None, ('dp', 'ep'))
- topk_idx: int32 [2, 4096, 6], P(None, ('dp', 'ep'))
- slot_idx: int32 [2, 4096, 6], P(None, ('dp', 'ep'))
- x_dispatch: bfloat16 [2, 64, 512, 1536], P(None, ('dp', 'ep'))
- h1_pre: bfloat16 [2, 64, 512, 512], P(None, ('dp', 'ep'))
- h3_pre: bfloat16 [2, 64, 512, 512], P(None, ('dp', 'ep'))
- w_gate: bfloat16 [64, 1536, 512], P('ep')
- w_up: bfloat16 [64, 1536, 512], P('ep')
- w_down: bfloat16 [64, 512, 1536], P('ep')
Outputs:
- output 1: bfloat16 [2, 4096, 1536], P(None, ('dp', 'ep'))
- output 2: float32 [2, 4096, 6], P(None, ('dp', 'ep'))
- output 3: float32 [64, 1536, 512], P(('dp', 'ep'))
- output 4: float32 [64, 1536, 512], P(('dp', 'ep'))
- output 5: float32 [64, 512, 1536], P(('dp', 'ep'))
All inputs are finite; a program needn't handle non-finite values.
Results may differ from the reference program's by a relative error of at most 0.00867723.
Values are sent between devices in bfloat16 or wider.
A program may use at most 768 MiB of HBM per device.

```python
import jax
import jax.numpy as jnp
from jax import lax

GROUP_SIZE = 32
TOKENS = 128
EXPERTS = 64
TOP_K = 6
D_MODEL = 1536
D_FF = 512
MICRO_BATCHES = 2
CAPACITY = 8 * ((5 * TOKENS * TOP_K) // (32 * EXPERTS) + 1)
BUF_ROWS = GROUP_SIZE * CAPACITY
GROUP_TOKENS = GROUP_SIZE * TOKENS
TOTAL_ROWS = EXPERTS * BUF_ROWS


def route_tokens(rng_key):
    key_base, key_bias, key_hot = jax.random.split(rng_key, 3)
    base_score = jax.random.randint(key_base, (GROUP_SIZE, TOKENS, EXPERTS), 0, 1024)
    expert_bias = jax.random.randint(key_bias, (EXPERTS,), 0, 1024)
    hot_expert = jax.random.randint(key_hot, (GROUP_SIZE, 1, 1), 0, EXPERTS)
    expert_ids = jnp.arange(EXPERTS)
    forced = jnp.where((jnp.arange(TOKENS)[None, :, None] <= CAPACITY) & (expert_ids[None, None, :] == hot_expert), 4096, 0)
    score_int = (base_score + expert_bias + forced) * EXPERTS + expert_ids
    topk_idx = lax.top_k(score_int, TOP_K)[1].astype(jnp.int32)
    flat_choice = topk_idx.reshape(GROUP_SIZE, TOKENS * TOP_K)
    onehot = (flat_choice[:, :, None] == expert_ids).astype(jnp.int32)
    count_before = jnp.cumsum(onehot, axis=1) - onehot
    position = jnp.sum(count_before * onehot, axis=2).reshape(GROUP_SIZE, TOKENS, TOP_K)
    slot_idx = jnp.where(position < CAPACITY, position, -1).astype(jnp.int32)
    return topk_idx.reshape(GROUP_TOKENS, TOP_K), slot_idx.reshape(GROUP_TOKENS, TOP_K)


def buffer_rows(topk_idx, slot_idx):
    source = (jnp.arange(GROUP_TOKENS) // TOKENS)[:, None]
    flat_row = (topk_idx * GROUP_SIZE + source) * CAPACITY + slot_idx
    return jnp.where(slot_idx >= 0, flat_row, TOTAL_ROWS)


def scatter_rows(flat_row, values):
    row_width = values.shape[-1]
    buffer = jnp.zeros((TOTAL_ROWS + 1, row_width), jnp.bfloat16)
    buffer = buffer.at[flat_row.reshape(-1)].set(values.reshape(-1, row_width))
    return buffer[:TOTAL_ROWS].reshape(EXPERTS, BUF_ROWS, row_width)


def gather_rows(expert_rows, flat_row):
    row_width = expert_rows.shape[-1]
    padded = jnp.concatenate([expert_rows.reshape(TOTAL_ROWS, row_width), jnp.zeros((1, row_width), expert_rows.dtype)], axis=0)
    return padded[flat_row]


def expert_forward(operands):
    x_rows, w_gate_e, w_up_e, w_down_e = operands
    x_f32 = x_rows.astype(jnp.float32)
    h1_rows = jnp.einsum('mrd,df->mrf', x_f32, w_gate_e.astype(jnp.float32)).astype(jnp.bfloat16)
    h3_rows = jnp.einsum('mrd,df->mrf', x_f32, w_up_e.astype(jnp.float32)).astype(jnp.bfloat16)
    h1_f32 = h1_rows.astype(jnp.float32)
    activation = (h1_f32 * jax.nn.sigmoid(h1_f32) * h3_rows.astype(jnp.float32)).astype(jnp.bfloat16)
    y_rows = jnp.einsum('mrf,fd->mrd', activation.astype(jnp.float32), w_down_e.astype(jnp.float32)).astype(jnp.bfloat16)
    return h1_rows, h3_rows, y_rows


def saved_forward(x_home, topk_idx, slot_idx, w_gate, w_up, w_down):
    flat_row = jax.vmap(buffer_rows)(topk_idx, slot_idx)
    x_rep = jnp.broadcast_to(x_home[:, :, None, :], (MICRO_BATCHES, GROUP_TOKENS, TOP_K, D_MODEL))
    x_dispatch = jax.vmap(scatter_rows)(flat_row, x_rep)
    h1_e, h3_e, y_e = lax.map(expert_forward, (jnp.moveaxis(x_dispatch, 1, 0), w_gate, w_up, w_down))
    expert_out = jax.vmap(gather_rows)(jnp.moveaxis(y_e, 0, 1), flat_row)
    return x_dispatch, jnp.moveaxis(h1_e, 0, 1), jnp.moveaxis(h3_e, 0, 1), expert_out


def setup_inputs(seed: int = 0, part: int = 0) -> dict:
    root_key = jax.random.key(seed)
    key_shared, key_parts = jax.random.split(root_key)
    key_wg, key_wu, key_wd = jax.random.split(key_shared, 3)
    w_gate = (jax.random.normal(key_wg, (EXPERTS, D_MODEL, D_FF), jnp.float32) * D_MODEL ** -0.5).astype(jnp.bfloat16)
    w_up = (jax.random.normal(key_wu, (EXPERTS, D_MODEL, D_FF), jnp.float32) * D_MODEL ** -0.5).astype(jnp.bfloat16)
    w_down = (jax.random.normal(key_wd, (EXPERTS, D_FF, D_MODEL), jnp.float32) * D_FF ** -0.5).astype(jnp.bfloat16)
    key_part = jax.random.fold_in(key_parts, part)
    key_route, key_x, key_dy, key_gate = jax.random.split(key_part, 4)
    topk_idx, slot_idx = jax.vmap(route_tokens)(jax.random.split(key_route, MICRO_BATCHES))
    x_home = jax.random.normal(key_x, (MICRO_BATCHES, GROUP_TOKENS, D_MODEL), jnp.float32).astype(jnp.bfloat16)
    grad_out = jax.random.normal(key_dy, (MICRO_BATCHES, GROUP_TOKENS, D_MODEL), jnp.float32).astype(jnp.bfloat16)
    gate_vals = jax.random.uniform(key_gate, (MICRO_BATCHES, GROUP_TOKENS, TOP_K), jnp.float32, 0.25, 1.0)
    x_dispatch, h1_pre, h3_pre, expert_out = saved_forward(x_home, topk_idx, slot_idx, w_gate, w_up, w_down)
    return {'grad_out': grad_out, 'expert_out': expert_out, 'gate_vals': gate_vals, 'topk_idx': topk_idx, 'slot_idx': slot_idx, 'x_dispatch': x_dispatch, 'h1_pre': h1_pre, 'h3_pre': h3_pre, 'w_gate': w_gate, 'w_up': w_up, 'w_down': w_down}


def gate_grad(operands):
    dy_block, y_block = operands
    return jnp.einsum('td,tkd->tk', dy_block.astype(jnp.float32), y_block.astype(jnp.float32))


def expert_backward(operands):
    x_rows, h1_rows, h3_rows, dy_rows, w_gate_e, w_up_e, w_down_e = operands
    h1_f32 = h1_rows.astype(jnp.float32)
    h3_f32 = h3_rows.astype(jnp.float32)
    sigmoid_h1 = jax.nn.sigmoid(h1_f32)
    silu_h1 = h1_f32 * sigmoid_h1
    activation = (silu_h1 * h3_f32).astype(jnp.bfloat16)
    dy_f32 = dy_rows.astype(jnp.float32)
    x_f32 = x_rows.astype(jnp.float32)
    grad_act = jnp.einsum('mrd,fd->mrf', dy_f32, w_down_e.astype(jnp.float32)).astype(jnp.bfloat16).astype(jnp.float32)
    grad_h1 = (grad_act * h3_f32 * sigmoid_h1 * (1.0 + h1_f32 * (1.0 - sigmoid_h1))).astype(jnp.bfloat16)
    grad_h3 = (grad_act * silu_h1).astype(jnp.bfloat16)
    g_down = jnp.einsum('mrf,mrd->fd', activation.astype(jnp.float32), dy_f32)
    g_gate = jnp.einsum('mrd,mrf->df', x_f32, grad_h1.astype(jnp.float32))
    g_up = jnp.einsum('mrd,mrf->df', x_f32, grad_h3.astype(jnp.float32))
    dx_rows = (jnp.einsum('mrf,df->mrd', grad_h1.astype(jnp.float32), w_gate_e.astype(jnp.float32)) + jnp.einsum('mrf,df->mrd', grad_h3.astype(jnp.float32), w_up_e.astype(jnp.float32))).astype(jnp.bfloat16)
    return g_gate, g_up, g_down, dx_rows


def reference(grad_out, expert_out, gate_vals, topk_idx, slot_idx, x_dispatch, h1_pre, h3_pre, w_gate, w_up, w_down):
    blocks = MICRO_BATCHES * GROUP_SIZE
    grad_gate = lax.map(gate_grad, (grad_out.reshape(blocks, TOKENS, D_MODEL), expert_out.reshape(blocks, TOKENS, TOP_K, D_MODEL)))
    grad_gate = grad_gate.reshape(MICRO_BATCHES, GROUP_TOKENS, TOP_K)
    flat_row = jax.vmap(buffer_rows)(topk_idx, slot_idx)
    gated_rows = (gate_vals[:, :, :, None] * grad_out[:, :, None, :].astype(jnp.float32)).astype(jnp.bfloat16)
    dy_dispatch = jax.vmap(scatter_rows)(flat_row, gated_rows)
    grad_w_gate, grad_w_up, grad_w_down, dx_rows = lax.map(expert_backward, (jnp.moveaxis(x_dispatch, 1, 0), jnp.moveaxis(h1_pre, 1, 0), jnp.moveaxis(h3_pre, 1, 0), jnp.moveaxis(dy_dispatch, 1, 0), w_gate, w_up, w_down))
    returned = jax.vmap(gather_rows)(jnp.moveaxis(dx_rows, 0, 1), flat_row)
    grad_x = jnp.sum(returned.astype(jnp.float32), axis=2).astype(jnp.bfloat16)
    return (grad_x, grad_gate, grad_w_gate, grad_w_up, grad_w_down)
```

```python
import functools
import jax
import jax.numpy as jnp
from jax import lax
from jax.experimental import pallas as pl
from jax.experimental.pallas import tpu as pltpu
from jax.sharding import PartitionSpec as P

MESH = pl.DeviceIdType.MESH
BF16 = jnp.bfloat16
F32 = jnp.float32
RETURN_ORDER = ((1, 0), (3, 0), (0, 1), (0, 3), (2, 0), (0, 2), (1, 1), (3, 3), (1, 3), (3, 1),
                (2, 1), (1, 2), (2, 3), (3, 2), (2, 2))


def exchange_kernel(n_dev, side, n_micro, tokens, top_k, d_model, d_ff, capacity,
                    dy_hbm, yd_hbm, gate_ref, topk_ref, slot_ref, h1_hbm, h3_hbm, w1_hbm, w3_hbm, w2_hbm,
                    dx_ref, dg_ref, dyd_hbm, dh1_hbm, dh3_hbm, act_hbm,
                    full, leaf, sib, dyd, dxs, ret, route, pad, w1, w3, w2, h1, h3, act_v, onehot, ybuf,
                    full_recv, full_send, leaf_send, sib_send, dyd_recv, route_send, route_recv,
                    ret_send, ret_recv, load_sem, y_sem, out_sem):
    me = lax.axis_index('ep')
    core = me % 2
    chip_x = (me // 2) % side
    chip_y = me // (2 * side)
    rows_dev = 2 * capacity
    half = d_model // 2

    def device(da, db, which):
        dx = da * (1 - core) + db * core
        dy = da * core + db * (1 - core)
        return (((chip_y + dy + 2 * side) % side) * side + (chip_x + dx + 2 * side) % side) * 2 + which

    def load_own(m, h):
        return pltpu.make_async_copy(dy_hbm.at[m, :, pl.ds(h * half, half)], full.at[m, h, 0], full_recv.at[m, h, 0])

    for m in range(n_micro):
        for h in range(2):
            load_own(m, h).start()
    loads = [pltpu.make_async_copy(src, dst, load_sem.at[i]) for i, (src, dst) in enumerate(
        ((w2_hbm, w2), (h1_hbm, h1), (h3_hbm, h3), (w1_hbm, w1), (w3_hbm, w3)))]

    barrier = pltpu.get_barrier_semaphore()

    def greet(k, carry):
        pl.semaphore_signal(barrier, inc=1, device_id={'ep': (me + k) % n_dev}, device_id_type=MESH)
        return carry

    lax.fori_loop(1, n_dev, greet, 0)
    for c in loads:
        c.start()

    for m in range(n_micro):
        pad[...] = jnp.zeros_like(pad)
        key = jnp.where(slot_ref[m] >= 0, topk_ref[m] * capacity + slot_ref[m], -1)
        pad[:, 0:top_k] = key.astype(F32)
        pad[:, 8:8 + top_k] = gate_ref[m]
        route[me, m] = jnp.transpose(pad[...])[0:16, :]
    pl.semaphore_wait(barrier, n_dev - 1)

    def send_route(da, db):
        pltpu.make_async_remote_copy(route.at[me], route.at[me], route_send, route_recv,
                                     device_id={'ep': device(da, db, core)}, device_id_type=MESH).start()

    n_route = 0
    for da, db in ((1, 0), (side - 1, 0), (2, 0), (0, 1), (0, side - 1), (1, 1), (1, side - 1), (side - 1, 1),
                   (side - 1, side - 1), (2, 1), (2, side - 1)):
        send_route(da, db)
        n_route += 1

    def send_full(m, h, ev, da, db, slot):
        pltpu.make_async_remote_copy(full.at[m, h, ev], full.at[m, h, slot], full_send, full_recv.at[m, h, slot],
                                     device_id={'ep': device(da, db, core)}, device_id_type=MESH).start()

    def item(m, i):
        h = i % 2
        ev = i // 2
        s = 1 - 2 * h
        pltpu.make_async_copy(full.at[m, h, ev], full.at[m, h, ev], full_recv.at[m, h, ev]).wait()

        @pl.when(ev == 0)
        def _():
            send_full(m, h, ev, s, 0, 1)
            send_full(m, h, ev, -s, 0, 2)

        @pl.when(ev == 1)
        def _():
            send_full(m, h, ev, s, 0, 3)

        @pl.when(ev < 4)
        def _():
            send_full(m, h, ev, 0, s, 4 + ev)

        k = ev % 4
        lvl = ev // 4
        da = (k % 2) * (1 - k // 2) * (-s) + (k // 2) * (1 - k % 2) * s + (k // 2) * (k % 2) * 2
        home = device(da, -s * lvl, core)
        leaf_chip = device(0, s * (2 * lvl - 1), 0)
        row = lax.broadcasted_iota(jnp.int32, (4 * rows_dev, tokens), 0)
        block = row // rows_dev
        inner = row - block * rows_dev
        dev = jnp.where(block == 0, me, jnp.where(block == 1, me + 1 - 2 * core,
                                                  jnp.where(block == 2, leaf_chip, leaf_chip + 1)))
        want = (dev * rows_dev + inner).astype(F32)
        table = route[home, m]
        pick = jnp.zeros((4 * rows_dev, tokens), F32)
        gate = jnp.zeros((4 * rows_dev, tokens), F32)
        for j in range(top_k):
            hit = want == table[j:j + 1, :]
            pick = jnp.where(hit, 1.0, pick)
            gate = jnp.where(hit, table[8 + j:9 + j, :], gate)
        gate = jnp.sum(gate, axis=1, keepdims=True)
        rows = jnp.dot(pick.astype(BF16), full[m, h, ev], preferred_element_type=F32)
        rows = (rows * gate).astype(BF16)
        leaf[m, h, ev] = rows[2 * rows_dev:].reshape(2, 2, capacity, half)
        sib[m, h, ev] = rows[rows_dev:2 * rows_dev].reshape(2, capacity, half)
        row0 = pl.multiple_of(home * capacity, capacity)
        col0 = pl.multiple_of(h * half, half)
        dyd[m, :, pl.ds(row0, capacity), pl.ds(col0, half)] = rows[:rows_dev].reshape(2, capacity, half)
        target = dyd.at[m, :, pl.ds(row0, capacity), pl.ds(col0, half)]
        for c in range(2):
            pltpu.make_async_remote_copy(leaf.at[m, h, ev, c], target, leaf_send, dyd_recv.at[m],
                                         device_id={'ep': leaf_chip + c}, device_id_type=MESH).start()
        pltpu.make_async_remote_copy(sib.at[m, h, ev], target, sib_send, dyd_recv.at[m],
                                     device_id={'ep': me + 1 - 2 * core}, device_id_type=MESH).start()

    def items(m, lo, hi):
        lax.fori_loop(lo, hi, lambda i, c: (item(m, i), c)[1], 0)

    chunk = 256
    per_exp = (n_dev * capacity) // chunk

    def compute(m, c):
        e = c // per_exp
        r0 = pl.multiple_of((c % per_exp) * chunk, chunk)
        nt = (((1,), (1,)), ((), ()))
        grad_act = lax.dot_general(dyd[m, e, pl.ds(r0, chunk)], w2[e], nt, preferred_element_type=F32)
        grad_act = grad_act.astype(BF16).astype(F32)
        h1_f32 = h1[m, e, pl.ds(r0, chunk)].astype(F32)
        h3_f32 = h3[m, e, pl.ds(r0, chunk)].astype(F32)
        sig = jax.nn.sigmoid(h1_f32)
        silu = h1_f32 * sig
        act = (silu * h3_f32).astype(BF16)
        grad_h1 = (grad_act * h3_f32 * sig * (1.0 + h1_f32 * (1.0 - sig))).astype(BF16)
        grad_h3 = (grad_act * silu).astype(BF16)
        rows = lax.dot_general(grad_h1, w1[e], nt, preferred_element_type=F32)
        rows = rows + lax.dot_general(grad_h3, w3[e], nt, preferred_element_type=F32)
        dxs[m, e, pl.ds(r0, chunk)] = rows.astype(BF16)
        h1[m, e, pl.ds(r0, chunk)] = grad_h1
        h3[m, e, pl.ds(r0, chunk)] = grad_h3
        act_v[m, e, pl.ds(r0, chunk)] = act

    def send_return(m):
        for which in range(2):
            for dx, dy in RETURN_ORDER:
                dst = (((chip_y + dy) % side) * side + (chip_x + dx) % side) * 2 + (core + which) % 2
                send_row(m, dst)
            if which == 0:
                send_row(m, me + 1 - 2 * core)

    def send_row(m, dst):
        row0 = pl.multiple_of(dst * capacity, capacity)
        pltpu.make_async_remote_copy(dxs.at[m, :, pl.ds(row0, capacity)], ret.at[m, me], ret_send, ret_recv.at[m],
                                     device_id={'ep': dst}, device_id_type=MESH).start()

    def out_copies(m):
        return [pltpu.make_async_copy(src.at[m], dst.at[m], out_sem.at[m, i]) for i, (src, dst) in enumerate(
            ((dyd, dyd_hbm), (h1, dh1_hbm), (h3, dh3_hbm), (act_v, act_hbm)))]

    def combine(m):
        key = jnp.where(slot_ref[m] >= 0, topk_ref[m] * capacity + slot_ref[m], -1)
        lane = lax.broadcasted_iota(jnp.int32, (tokens, n_dev * rows_dev), 1)
        mat = jnp.zeros((tokens, n_dev * rows_dev), F32)
        for j in range(top_k):
            mat = jnp.where(lane == key[:, j:j + 1], 1.0, mat)
        onehot[m] = mat.astype(BF16)
        row0 = pl.multiple_of(me * capacity, capacity)
        ret[m, me] = dxs[m, :, pl.ds(row0, capacity)]
        pltpu.make_async_copy(ret.at[m, pl.ds(0, n_dev - 1)], ret.at[m, pl.ds(0, n_dev - 1)], ret_recv.at[m]).wait()
        for c in range(0, d_model, 512):
            back = ret[m, :, :, :, c:c + 512].reshape(n_dev * rows_dev, 512)
            dx_ref[m, :, c:c + 512] = jnp.dot(onehot[m], back, preferred_element_type=F32).astype(BF16)

    pltpu.make_async_copy(route.at[pl.ds(0, n_route)], route.at[pl.ds(0, n_route)], route_recv).wait()
    items(0, 0, 8)
    items(1, 0, 2)
    items(0, 8, 16)
    items(1, 2, 8)

    def wait_dyd(m):
        part = dyd.at[m, :, pl.ds(0, (n_dev - 8) * capacity)]
        pltpu.make_async_copy(part, part, dyd_recv.at[m]).wait()

    for c in loads:
        c.wait()
    wait_dyd(0)

    def mixed(c, carry):
        compute(0, c)
        item(1, 8 + 2 * c)
        item(1, 9 + 2 * c)
        return carry

    lax.fori_loop(0, 2 * per_exp, mixed, 0)
    send_return(0)
    wait_dyd(1)
    lax.fori_loop(0, 2 * per_exp, lambda c, carry: (compute(1, c), carry)[1], 0)
    send_return(1)
    outs = out_copies(0) + out_copies(1)
    for c in outs:
        c.start()

    t_blk = ybuf.shape[1]
    n_blk = tokens // t_blk

    def y_copy(i):
        m = i // n_blk
        t0 = (i % n_blk) * t_blk
        return pltpu.make_async_copy(yd_hbm.at[m, pl.ds(t0, t_blk)], ybuf.at[i % 2], y_sem.at[i % 2])

    y_copy(0).start()

    def gate_grad(i, carry):
        @pl.when(i + 1 < n_micro * n_blk)
        def _():
            y_copy(i + 1).start()

        y_copy(i).wait()
        m = i // n_blk
        t0 = pl.multiple_of((i % n_blk) * t_blk, t_blk)
        total = jnp.zeros((t_blk, top_k), F32)
        for h in range(2):
            dy_blk = full[m, h, 0, pl.ds(t0, t_blk), :].astype(F32)
            y_blk = ybuf[i % 2, :, :, h * half:(h + 1) * half].astype(F32)
            total = total + jnp.sum(y_blk * dy_blk[:, None, :], axis=-1)
        dg_ref[m, pl.ds(t0, t_blk), :] = total
        return carry

    lax.fori_loop(0, n_micro * n_blk, gate_grad, 0)
    for m in range(n_micro):
        combine(m)
    for c in outs:
        c.wait()
    sent = full.at[:, :, pl.ds(0, 7)]
    pltpu.make_async_copy(sent, sent, full_send).wait()
    pltpu.make_async_copy(leaf, leaf, leaf_send).wait()
    pltpu.make_async_copy(sib, sib, sib_send).wait()
    pltpu.make_async_copy(route.at[pl.ds(0, n_route)], route.at[pl.ds(0, n_route)], route_send).wait()
    pltpu.make_async_copy(ret.at[:, pl.ds(0, n_dev - 1)], ret.at[:, pl.ds(0, n_dev - 1)], ret_send).wait()


def solution(mesh):
    n_dev = mesh.shape['ep']
    side = 1
    while 2 * side * side < n_dev:
        side += 1
    tok_spec = P(None, ('dp', 'ep'))
    w_spec = P('ep')
    grad_w_spec = P(('dp', 'ep'))

    def local_step(grad_out, expert_out, gate_vals, topk_idx, slot_idx, x_dispatch, h1_pre, h3_pre, w_gate, w_up, w_down):
        n_micro, tokens, top_k, d_model = expert_out.shape
        local_exp, _, d_ff = w_gate.shape
        rows = x_dispatch.shape[2]
        capacity = rows // n_dev
        half = d_model // 2
        hbm = pl.BlockSpec(memory_space=pl.ANY)
        vmem = pl.BlockSpec(memory_space=pltpu.VMEM)
        dma = pltpu.SemaphoreType.DMA
        kernel = functools.partial(exchange_kernel, n_dev, side, n_micro, tokens, top_k, d_model, d_ff, capacity)
        ff_shape = (n_micro, local_exp, rows, d_ff)
        wide_shape = (n_micro, local_exp, rows, d_model)
        grad_x, grad_gate, dyd, grad_h1, grad_h3, act = pl.pallas_call(
            kernel,
            name='exchange',
            out_shape=(
                jax.ShapeDtypeStruct((n_micro, tokens, d_model), BF16),
                jax.ShapeDtypeStruct((n_micro, tokens, top_k), F32),
                jax.ShapeDtypeStruct(wide_shape, BF16),
                jax.ShapeDtypeStruct(ff_shape, BF16),
                jax.ShapeDtypeStruct(ff_shape, BF16),
                jax.ShapeDtypeStruct(ff_shape, BF16),
            ),
            in_specs=[hbm, hbm, vmem, vmem, vmem, hbm, hbm, hbm, hbm, hbm],
            out_specs=(vmem, vmem, hbm, hbm, hbm, hbm),
            scratch_shapes=[
                pltpu.VMEM((n_micro, 2, 8, tokens, half), BF16),
                pltpu.VMEM((n_micro, 2, 8, 2, local_exp, capacity, half), BF16),
                pltpu.VMEM((n_micro, 2, 8, local_exp, capacity, half), BF16),
                pltpu.VMEM(wide_shape, BF16),
                pltpu.VMEM(wide_shape, BF16),
                pltpu.VMEM((n_micro, n_dev, local_exp, capacity, d_model), BF16),
                pltpu.VMEM((n_dev, n_micro, 16, tokens), F32),
                pltpu.VMEM((tokens, 128), F32),
                pltpu.VMEM(w_gate.shape, BF16),
                pltpu.VMEM(w_up.shape, BF16),
                pltpu.VMEM(w_down.shape, BF16),
                pltpu.VMEM(ff_shape, BF16),
                pltpu.VMEM(ff_shape, BF16),
                pltpu.VMEM(ff_shape, BF16),
                pltpu.VMEM((n_micro, tokens, n_dev * local_exp * capacity), BF16),
                pltpu.VMEM((2, 16, top_k, d_model), BF16),
                dma((n_micro, 2, 8)),
                dma, dma, dma,
                dma((n_micro,)),
                dma, dma, dma,
                dma((n_micro,)),
                dma((5,)),
                dma((2,)),
                dma((n_micro, 4)),
            ],
            compiler_params=pltpu.CompilerParams(collective_id=0, has_side_effects=True, vmem_limit_bytes=67043328),
            cost_estimate=pl.CostEstimate(flops=10 ** 10, bytes_accessed=5 * 10 ** 7, transcendentals=0),
        )(grad_out, expert_out, gate_vals, topk_idx, slot_idx, h1_pre, h3_pre, w_gate, w_up, w_down)
        grad_w_gate = jnp.einsum('merd,merf->edf', x_dispatch, grad_h1, preferred_element_type=F32)
        grad_w_up = jnp.einsum('merd,merf->edf', x_dispatch, grad_h3, preferred_element_type=F32)
        grad_w_down = jnp.einsum('merf,merd->efd', act, dyd, preferred_element_type=F32)
        return grad_x, grad_gate, grad_w_gate, grad_w_up, grad_w_down

    in_specs = (tok_spec,) * 8 + (w_spec,) * 3
    out_specs = (tok_spec, tok_spec, grad_w_spec, grad_w_spec, grad_w_spec)
    return jax.shard_map(local_step, mesh=mesh, in_specs=in_specs, out_specs=out_specs, check_vma=False)
```

```python
import functools
import jax
import jax.numpy as jnp
from jax import lax
from jax.experimental import pallas as pl
from jax.experimental.pallas import tpu as pltpu
from jax.sharding import PartitionSpec as P

MESH = pl.DeviceIdType.MESH
BF16 = jnp.bfloat16
F32 = jnp.float32
RETURN_ORDER = ((1, 0), (3, 0), (0, 1), (0, 3), (2, 0), (0, 2), (1, 1), (3, 3), (1, 3), (3, 1),
                (2, 1), (1, 2), (2, 3), (3, 2), (2, 2))


def exchange_kernel(n_dev, side, n_micro, tokens, top_k, d_model, d_ff, capacity,
                    dy_hbm, yd_hbm, gate_ref, topk_ref, slot_ref, h1_hbm, h3_hbm, w1_hbm, w3_hbm, w2_hbm,
                    dx_ref, dg_ref, dyd_hbm, dh1_hbm, dh3_hbm, act_hbm,
                    full, leaf, sib, dyd, dxs, ret, route, pad, w1, w3, w2, h1, h3, act_v, onehot, ybuf,
                    full_recv, full_send, leaf_send, sib_send, dyd_recv, route_send, route_recv,
                    ret_send, ret_recv, load_sem, y_sem, out_sem):
    me = lax.axis_index('ep')
    core = me % 2
    chip_x = (me // 2) % side
    chip_y = me // (2 * side)
    rows_dev = 2 * capacity
    half = d_model // 2

    def device(da, db, which):
        dx = da * (1 - core) + db * core
        dy = da * core + db * (1 - core)
        return (((chip_y + dy + 2 * side) % side) * side + (chip_x + dx + 2 * side) % side) * 2 + which

    def load_own(m, h):
        return pltpu.make_async_copy(dy_hbm.at[m, :, pl.ds(h * half, half)], full.at[m, h, 0], full_recv.at[m, h, 0])

    for m in range(n_micro):
        for h in range(2):
            load_own(m, h).start()
    loads = [pltpu.make_async_copy(src, dst, load_sem.at[i]) for i, (src, dst) in enumerate(
        ((w2_hbm, w2), (h1_hbm, h1), (h3_hbm, h3), (w1_hbm, w1), (w3_hbm, w3)))]

    barrier = pltpu.get_barrier_semaphore()

    def greet(k, carry):
        pl.semaphore_signal(barrier, inc=1, device_id={'ep': (me + k) % n_dev}, device_id_type=MESH)
        return carry

    lax.fori_loop(1, n_dev, greet, 0)
    for c in loads:
        c.start()

    for m in range(n_micro):
        slot = slot_ref[:, m, :]
        key = jnp.where(slot >= 0, topk_ref[:, m, :] * capacity + slot, -1)
        route[me, m] = jnp.zeros((16, tokens), F32)
        route[me, m, 0:top_k] = key.astype(F32)
        route[me, m, 8:8 + top_k] = gate_ref[:, m, :]
    pl.semaphore_wait(barrier, n_dev - 1)

    def send_route(da, db):
        pltpu.make_async_remote_copy(route.at[me], route.at[me], route_send, route_recv,
                                     device_id={'ep': device(da, db, core)}, device_id_type=MESH).start()

    n_route = 0
    for da, db in ((1, 0), (side - 1, 0), (2, 0), (0, 1), (0, side - 1), (1, 1), (1, side - 1), (side - 1, 1),
                   (side - 1, side - 1), (2, 1), (2, side - 1)):
        send_route(da, db)
        n_route += 1

    def send_full(m, h, ev, da, db, slot):
        pltpu.make_async_remote_copy(full.at[m, h, ev], full.at[m, h, slot], full_send, full_recv.at[m, h, slot],
                                     device_id={'ep': device(da, db, core)}, device_id_type=MESH).start()

    def item(m, i):
        h = i % 2
        ev = i // 2
        s = 1 - 2 * h
        pltpu.make_async_copy(full.at[m, h, ev], full.at[m, h, ev], full_recv.at[m, h, ev]).wait()

        @pl.when(ev == 0)
        def _():
            send_full(m, h, ev, s, 0, 1)
            send_full(m, h, ev, -s, 0, 2)

        @pl.when(ev == 1)
        def _():
            send_full(m, h, ev, s, 0, 3)

        @pl.when(ev < 4)
        def _():
            send_full(m, h, ev, 0, s, 4 + ev)

        k = ev % 4
        lvl = ev // 4
        da = (k % 2) * (1 - k // 2) * (-s) + (k // 2) * (1 - k % 2) * s + (k // 2) * (k % 2) * 2
        home = device(da, -s * lvl, core)
        leaf_chip = device(0, s * (2 * lvl - 1), 0)
        row = lax.broadcasted_iota(jnp.int32, (4 * rows_dev, tokens), 0)
        block = row // rows_dev
        inner = row - block * rows_dev
        dev = jnp.where(block == 0, me, jnp.where(block == 1, me + 1 - 2 * core,
                                                  jnp.where(block == 2, leaf_chip, leaf_chip + 1)))
        want = (dev * rows_dev + inner).astype(F32)
        table = route[home, m]
        pick = jnp.zeros((4 * rows_dev, tokens), F32)
        gate = jnp.zeros((4 * rows_dev, tokens), F32)
        for j in range(top_k):
            hit = want == table[j:j + 1, :]
            pick = jnp.where(hit, 1.0, pick)
            gate = jnp.where(hit, table[8 + j:9 + j, :], gate)
        gate = jnp.sum(gate, axis=1, keepdims=True)
        rows = jnp.dot(pick.astype(BF16), full[m, h, ev], preferred_element_type=F32)
        rows = (rows * gate).astype(BF16)
        leaf[m, h, ev] = rows[2 * rows_dev:].reshape(2, 2, capacity, half)
        sib[m, h, ev] = rows[rows_dev:2 * rows_dev].reshape(2, capacity, half)
        row0 = pl.multiple_of(home * capacity, capacity)
        col0 = pl.multiple_of(h * half, half)
        dyd[m, :, pl.ds(row0, capacity), pl.ds(col0, half)] = rows[:rows_dev].reshape(2, capacity, half)
        target = dyd.at[m, :, pl.ds(row0, capacity), pl.ds(col0, half)]
        for c in range(2):
            pltpu.make_async_remote_copy(leaf.at[m, h, ev, c], target, leaf_send, dyd_recv.at[m],
                                         device_id={'ep': leaf_chip + c}, device_id_type=MESH).start()
        pltpu.make_async_remote_copy(sib.at[m, h, ev], target, sib_send, dyd_recv.at[m],
                                     device_id={'ep': me + 1 - 2 * core}, device_id_type=MESH).start()

    def items(m, lo, hi):
        lax.fori_loop(lo, hi, lambda i, c: (item(m, i), c)[1], 0)

    chunk = 256
    per_exp = (n_dev * capacity) // chunk

    def compute(m, c):
        e = c // per_exp
        r0 = pl.multiple_of((c % per_exp) * chunk, chunk)
        nt = (((1,), (1,)), ((), ()))
        grad_act = lax.dot_general(dyd[m, e, pl.ds(r0, chunk)], w2[e], nt, preferred_element_type=F32)
        grad_act = grad_act.astype(BF16).astype(F32)
        h1_f32 = h1[m, e, pl.ds(r0, chunk)].astype(F32)
        h3_f32 = h3[m, e, pl.ds(r0, chunk)].astype(F32)
        sig = jax.nn.sigmoid(h1_f32)
        silu = h1_f32 * sig
        act = (silu * h3_f32).astype(BF16)
        grad_h1 = (grad_act * h3_f32 * sig * (1.0 + h1_f32 * (1.0 - sig))).astype(BF16)
        grad_h3 = (grad_act * silu).astype(BF16)
        rows = lax.dot_general(grad_h1, w1[e], nt, preferred_element_type=F32)
        rows = rows + lax.dot_general(grad_h3, w3[e], nt, preferred_element_type=F32)
        dxs[m, e, pl.ds(r0, chunk)] = rows.astype(BF16)
        h1[m, e, pl.ds(r0, chunk)] = grad_h1
        h3[m, e, pl.ds(r0, chunk)] = grad_h3
        act_v[m, e, pl.ds(r0, chunk)] = act

    def send_return(m):
        for which in range(2):
            for dx, dy in RETURN_ORDER:
                dst = (((chip_y + dy) % side) * side + (chip_x + dx) % side) * 2 + (core + which) % 2
                send_row(m, dst)
            if which == 0:
                send_row(m, me + 1 - 2 * core)

    def send_row(m, dst):
        row0 = pl.multiple_of(dst * capacity, capacity)
        pltpu.make_async_remote_copy(dxs.at[m, :, pl.ds(row0, capacity)], ret.at[m, me], ret_send, ret_recv.at[m],
                                     device_id={'ep': dst}, device_id_type=MESH).start()

    def out_copies(m):
        return [pltpu.make_async_copy(src.at[m], dst.at[m], out_sem.at[m, i]) for i, (src, dst) in enumerate(
            ((dyd, dyd_hbm), (h1, dh1_hbm), (h3, dh3_hbm), (act_v, act_hbm)))]

    def combine(m):
        pad[...] = jnp.zeros_like(pad)
        pad[0:16] = route[me, m]
        key = jnp.transpose(pad[...])
        place = lax.broadcasted_iota(jnp.int32, (tokens, n_dev * rows_dev), 1).astype(F32)
        mat = jnp.zeros((tokens, n_dev * rows_dev), F32)
        for j in range(top_k):
            mat = jnp.where(place == key[:, j:j + 1], 1.0, mat)
        onehot[m] = mat.astype(BF16)
        row0 = pl.multiple_of(me * capacity, capacity)
        ret[m, me] = dxs[m, :, pl.ds(row0, capacity)]
        pltpu.make_async_copy(ret.at[m, pl.ds(0, n_dev - 1)], ret.at[m, pl.ds(0, n_dev - 1)], ret_recv.at[m]).wait()
        for c in range(0, d_model, 512):
            back = ret[m, :, :, :, c:c + 512].reshape(n_dev * rows_dev, 512)
            dx_ref[m, :, c:c + 512] = jnp.dot(onehot[m], back, preferred_element_type=F32).astype(BF16)

    pltpu.make_async_copy(route.at[pl.ds(0, n_route)], route.at[pl.ds(0, n_route)], route_recv).wait()
    items(0, 0, 8)
    items(1, 0, 2)
    items(0, 8, 16)
    items(1, 2, 8)

    def wait_dyd(m):
        part = dyd.at[m, :, pl.ds(0, (n_dev - 8) * capacity)]
        pltpu.make_async_copy(part, part, dyd_recv.at[m]).wait()

    for c in loads:
        c.wait()
    wait_dyd(0)

    def mixed(c, carry):
        compute(0, c)
        item(1, 8 + 2 * c)
        item(1, 9 + 2 * c)
        return carry

    lax.fori_loop(0, 2 * per_exp, mixed, 0)
    send_return(0)
    wait_dyd(1)
    lax.fori_loop(0, 2 * per_exp, lambda c, carry: (compute(1, c), carry)[1], 0)
    send_return(1)
    outs = out_copies(0) + out_copies(1)
    for c in outs:
        c.start()

    def y_copy(i):
        return pltpu.make_async_copy(yd_hbm.at[i // top_k, i % top_k], ybuf.at[i % 2], y_sem.at[i % 2])

    y_copy(0).start()
    lane = lax.broadcasted_iota(jnp.int32, (tokens, 128), 1)
    for m in range(n_micro):
        def gate_grad(j, total, m=m):
            i = m * top_k + j

            @pl.when(i + 1 < n_micro * top_k)
            def _():
                y_copy(i + 1).start()

            y_copy(i).wait()
            part = jnp.zeros((tokens, 128), F32)
            for c in range(0, d_model, 128):
                dy_blk = full[m, c // half, 0, :, c % half:c % half + 128].astype(F32)
                part = part + dy_blk * ybuf[i % 2, :, c:c + 128].astype(F32)
            return jnp.where(lane == j, jnp.sum(part, axis=1, keepdims=True), total)

        total = lax.fori_loop(0, top_k, gate_grad, jnp.zeros((tokens, 128), F32))
        dg_ref[:, m, :] = jnp.transpose(total)[0:top_k, :]
    for m in range(n_micro):
        combine(m)
    for c in outs:
        c.wait()
    sent = full.at[:, :, pl.ds(0, 7)]
    pltpu.make_async_copy(sent, sent, full_send).wait()
    pltpu.make_async_copy(leaf, leaf, leaf_send).wait()
    pltpu.make_async_copy(sib, sib, sib_send).wait()
    pltpu.make_async_copy(route.at[pl.ds(0, n_route)], route.at[pl.ds(0, n_route)], route_send).wait()
    pltpu.make_async_copy(ret.at[:, pl.ds(0, n_dev - 1)], ret.at[:, pl.ds(0, n_dev - 1)], ret_send).wait()


def weight_kernel(x_ref, g1_ref, g3_ref, act_ref, dy_ref, o1_ref, o3_ref, o2_ref):
    tn = (((0,), (0,)), ((), ()))

    def flat(ref):
        return ref[...].reshape(-1, ref.shape[-1])

    x = flat(x_ref)
    o1_ref[0] = lax.dot_general(x, flat(g1_ref), tn, preferred_element_type=F32)
    o3_ref[0] = lax.dot_general(x, flat(g3_ref), tn, preferred_element_type=F32)
    o2_ref[0] = lax.dot_general(flat(act_ref), flat(dy_ref), tn, preferred_element_type=F32)


def weight_grads(x, g1, g3, act, dy):
    n_micro, local_exp, rows, d_model = x.shape
    d_ff = g1.shape[-1]
    tile = 256
    wide = pl.BlockSpec((n_micro, 1, rows, tile), lambda e, t: (0, e, 0, t))
    narrow = pl.BlockSpec((n_micro, 1, rows, d_ff), lambda e, t: (0, e, 0, 0))
    tall = pl.BlockSpec((1, tile, d_ff), lambda e, t: (e, t, 0))
    return pl.pallas_call(
        weight_kernel,
        name='weight_grads',
        grid=(local_exp, d_model // tile),
        out_shape=(jax.ShapeDtypeStruct((local_exp, d_model, d_ff), F32),) * 2
        + (jax.ShapeDtypeStruct((local_exp, d_ff, d_model), F32),),
        in_specs=[wide, narrow, narrow, narrow, wide],
        out_specs=(tall, tall, pl.BlockSpec((1, d_ff, tile), lambda e, t: (e, 0, t))),
        compiler_params=pltpu.CompilerParams(vmem_limit_bytes=67043328),
    )(x, g1, g3, act, dy)


def solution(mesh):
    n_dev = mesh.shape['ep']
    side = 1
    while 2 * side * side < n_dev:
        side += 1
    tok_spec = P(None, ('dp', 'ep'))
    w_spec = P('ep')
    grad_w_spec = P(('dp', 'ep'))

    def local_step(grad_out, expert_out, gate_vals, topk_idx, slot_idx, x_dispatch, h1_pre, h3_pre, w_gate, w_up, w_down):
        n_micro, tokens, top_k, d_model = expert_out.shape
        local_exp, _, d_ff = w_gate.shape
        rows = x_dispatch.shape[2]
        capacity = rows // n_dev
        half = d_model // 2
        hbm = pl.BlockSpec(memory_space=pl.ANY)
        by_choice = functools.partial(jnp.transpose, axes=(2, 0, 1))
        vmem = pl.BlockSpec(memory_space=pltpu.VMEM)
        dma = pltpu.SemaphoreType.DMA
        kernel = functools.partial(exchange_kernel, n_dev, side, n_micro, tokens, top_k, d_model, d_ff, capacity)
        ff_shape = (n_micro, local_exp, rows, d_ff)
        wide_shape = (n_micro, local_exp, rows, d_model)
        grad_x, grad_gate, dyd, grad_h1, grad_h3, act = pl.pallas_call(
            kernel,
            name='exchange',
            out_shape=(
                jax.ShapeDtypeStruct((n_micro, tokens, d_model), BF16),
                jax.ShapeDtypeStruct((top_k, n_micro, tokens), F32),
                jax.ShapeDtypeStruct(wide_shape, BF16),
                jax.ShapeDtypeStruct(ff_shape, BF16),
                jax.ShapeDtypeStruct(ff_shape, BF16),
                jax.ShapeDtypeStruct(ff_shape, BF16),
            ),
            in_specs=[hbm, hbm, vmem, vmem, vmem, hbm, hbm, hbm, hbm, hbm],
            out_specs=(vmem, vmem, hbm, hbm, hbm, hbm),
            scratch_shapes=[
                pltpu.VMEM((n_micro, 2, 8, tokens, half), BF16),
                pltpu.VMEM((n_micro, 2, 8, 2, local_exp, capacity, half), BF16),
                pltpu.VMEM((n_micro, 2, 8, local_exp, capacity, half), BF16),
                pltpu.VMEM(wide_shape, BF16),
                pltpu.VMEM(wide_shape, BF16),
                pltpu.VMEM((n_micro, n_dev, local_exp, capacity, d_model), BF16),
                pltpu.VMEM((n_dev, n_micro, 16, tokens), F32),
                pltpu.VMEM((tokens, 128), F32),
                pltpu.VMEM(w_gate.shape, BF16),
                pltpu.VMEM(w_up.shape, BF16),
                pltpu.VMEM(w_down.shape, BF16),
                pltpu.VMEM(ff_shape, BF16),
                pltpu.VMEM(ff_shape, BF16),
                pltpu.VMEM(ff_shape, BF16),
                pltpu.VMEM((n_micro, tokens, n_dev * local_exp * capacity), BF16),
                pltpu.VMEM((2, tokens, d_model), BF16),
                dma((n_micro, 2, 8)),
                dma, dma, dma,
                dma((n_micro,)),
                dma, dma, dma,
                dma((n_micro,)),
                dma((5,)),
                dma((2,)),
                dma((n_micro, 4)),
            ],
            compiler_params=pltpu.CompilerParams(collective_id=0, has_side_effects=True, vmem_limit_bytes=67043328),
            cost_estimate=pl.CostEstimate(flops=10 ** 10, bytes_accessed=5 * 10 ** 7, transcendentals=0),
        )(grad_out, jnp.transpose(expert_out, (0, 2, 1, 3)), by_choice(gate_vals), by_choice(topk_idx), by_choice(slot_idx),
          h1_pre, h3_pre, w_gate, w_up, w_down)
        grad_gate = jnp.transpose(grad_gate, (1, 2, 0))
        grad_w_gate, grad_w_up, grad_w_down = weight_grads(x_dispatch, grad_h1, grad_h3, act, dyd)
        return grad_x, grad_gate, grad_w_gate, grad_w_up, grad_w_down

    in_specs = (tok_spec,) * 8 + (w_spec,) * 3
    out_specs = (tok_spec, tok_spec, grad_w_spec, grad_w_spec, grad_w_spec)
    return jax.shard_map(local_step, mesh=mesh, in_specs=in_specs, out_specs=out_specs, check_vma=False)
```

```python
import functools
import jax
import jax.numpy as jnp
from jax import lax
from jax.experimental import pallas as pl
from jax.experimental.pallas import tpu as pltpu
from jax.sharding import PartitionSpec as P

MESH = pl.DeviceIdType.MESH
BF16 = jnp.bfloat16
VMEM_GRANT = 67043328 - 19 * 2 ** 20
F32 = jnp.float32
RETURN_ORDER = ((1, 0), (3, 0), (0, 1), (0, 3), (2, 0), (0, 2), (1, 1), (3, 3), (1, 3), (3, 1),
                (2, 1), (1, 2), (2, 3), (3, 2), (2, 2))


def exchange_kernel(n_dev, side, n_micro, tokens, top_k, d_model, d_ff, capacity,
                    dy_hbm, yd_hbm, gate_ref, topk_ref, slot_ref, x_hbm, h1_hbm, h3_hbm, w1_hbm, w3_hbm, w2_hbm,
                    dx_ref, dg_ref, dw1_ref, dw3_ref, dw2_ref,
                    full, leaf, sib, dyd, dxs, ret, route, pad, w1, w3, w2, h1, h3, act_v, onehot,
                    full_recv, full_send, leaf_send, sib_send, dyd_recv, route_send, route_recv,
                    ret_send, ret_recv, load_sem, y_sem, x_sem):
    me = lax.axis_index('ep')
    core = me % 2
    chip_x = (me // 2) % side
    chip_y = me // (2 * side)
    rows_dev = 2 * capacity
    half = d_model // 2

    def device(da, db, which):
        dx = da * (1 - core) + db * core
        dy = da * core + db * (1 - core)
        return (((chip_y + dy + 2 * side) % side) * side + (chip_x + dx + 2 * side) % side) * 2 + which

    def load_own(m, h):
        return pltpu.make_async_copy(dy_hbm.at[m, :, pl.ds(h * half, half)], full.at[m, h, 0, 0], full_recv.at[m, h, 0])

    for m in range(n_micro):
        for h in range(2):
            load_own(m, h).start()
    loads = [pltpu.make_async_copy(src, dst, load_sem.at[i]) for i, (src, dst) in enumerate(
        ((w2_hbm, w2), (h1_hbm, h1), (h3_hbm, h3), (w1_hbm, w1), (w3_hbm, w3)))]

    barrier = pltpu.get_barrier_semaphore()

    def greet(k, carry):
        pl.semaphore_signal(barrier, inc=1, device_id={'ep': (me + k) % n_dev}, device_id_type=MESH)
        return carry

    lax.fori_loop(1, n_dev, greet, 0)
    for c in loads:
        c.start()

    for m in range(n_micro):
        slot = slot_ref[:, m, :]
        key = jnp.where(slot >= 0, topk_ref[:, m, :] * capacity + slot, -1)
        route[me, m] = jnp.zeros((16, tokens), F32)
        route[me, m, 0:top_k] = key.astype(F32)
        route[me, m, 8:8 + top_k] = gate_ref[:, m, :]
    pl.semaphore_wait(barrier, n_dev - 1)

    def send_route(da, db):
        pltpu.make_async_remote_copy(route.at[me], route.at[me], route_send, route_recv,
                                     device_id={'ep': device(da, db, core)}, device_id_type=MESH).start()

    n_route = 0
    for da, db in ((1, 0), (side - 1, 0), (2, 0), (0, 1), (0, side - 1), (1, 1), (1, side - 1), (side - 1, 1),
                   (side - 1, side - 1), (2, 1), (2, side - 1)):
        send_route(da, db)
        n_route += 1

    def send_full(m, h, ev, da, db, slot):
        pltpu.make_async_remote_copy(full.at[m, h, ev // 4, ev % 4], full.at[m, h, slot // 4, slot % 4],
                                     full_send.at[m], full_recv.at[m, h, slot],
                                     device_id={'ep': device(da, db, core)}, device_id_type=MESH).start()

    def item(m, i):
        h = i % 2
        ev = i // 2
        s = 1 - 2 * h
        k = ev % 4
        lvl = ev // 4
        tok = full.at[m, h, lvl, k]
        pltpu.make_async_copy(tok, tok, full_recv.at[m, h, ev]).wait()

        @pl.when(ev == 0)
        def _():
            send_full(m, h, ev, s, 0, 1)
            send_full(m, h, ev, -s, 0, 2)

        @pl.when(ev == 1)
        def _():
            send_full(m, h, ev, s, 0, 3)

        @pl.when(ev < 4)
        def _():
            send_full(m, h, ev, 0, s, 4 + ev)

        da = (k % 2) * (1 - k // 2) * (-s) + (k // 2) * (1 - k % 2) * s + (k // 2) * (k % 2) * 2
        home = device(da, -s * lvl, core)
        leaf_chip = device(0, s * (2 * lvl - 1), 0)
        row = lax.broadcasted_iota(jnp.int32, (4 * rows_dev, tokens), 0)
        block = row // rows_dev
        inner = row - block * rows_dev
        dev = jnp.where(block == 0, me, jnp.where(block == 1, me + 1 - 2 * core,
                                                  jnp.where(block == 2, leaf_chip, leaf_chip + 1)))
        want = (dev * rows_dev + inner).astype(F32)
        table = route[home, m]
        pick = jnp.zeros((4 * rows_dev, tokens), F32)
        gate = jnp.zeros((4 * rows_dev, tokens), F32)
        for j in range(top_k):
            hit = want == table[j:j + 1, :]
            pick = jnp.where(hit, 1.0, pick)
            gate = jnp.where(hit, table[8 + j:9 + j, :], gate)
        gate = jnp.sum(gate, axis=1, keepdims=True)
        rows = jnp.dot(pick.astype(BF16), tok[...], preferred_element_type=F32)
        rows = (rows * gate).astype(BF16)
        leaf[m, h, ev] = rows[2 * rows_dev:].reshape(2, 2, capacity, half)
        sib[m, h, ev] = rows[rows_dev:2 * rows_dev].reshape(2, capacity, half)
        row0 = pl.multiple_of(home * capacity, capacity)
        col0 = pl.multiple_of(h * half, half)
        dyd[m, :, pl.ds(row0, capacity), pl.ds(col0, half)] = rows[:rows_dev].reshape(2, capacity, half)
        target = dyd.at[m, :, pl.ds(row0, capacity), pl.ds(col0, half)]
        for c in range(2):
            pltpu.make_async_remote_copy(leaf.at[m, h, ev, c], target, leaf_send, dyd_recv.at[m],
                                         device_id={'ep': leaf_chip + c}, device_id_type=MESH).start()
        pltpu.make_async_remote_copy(sib.at[m, h, ev], target, sib_send, dyd_recv.at[m],
                                     device_id={'ep': me + 1 - 2 * core}, device_id_type=MESH).start()

    def items(m, lo, hi):
        lax.fori_loop(lo, hi, lambda i, c: (item(m, i), c)[1], 0)

    chunk = 256
    per_exp = (n_dev * capacity) // chunk

    def out_rows(m):
        return dxs if m == 0 else full.at[0]

    def own_rows(m, dst):
        row0 = pl.multiple_of((dst % (tokens // capacity)) * capacity, capacity)
        return out_rows(m).at[:, :, dst // (tokens // capacity), pl.ds(row0, capacity), :]

    def compute(m, c):
        e = c // per_exp
        r0 = pl.multiple_of((c % per_exp) * chunk, chunk)
        nt = (((1,), (1,)), ((), ()))
        grad_act = lax.dot_general(dyd[m, e, pl.ds(r0, chunk)], w2[e], nt, preferred_element_type=F32)
        grad_act = grad_act.astype(BF16).astype(F32)
        h1_f32 = h1[m, e, pl.ds(r0, chunk)].astype(F32)
        h3_f32 = h3[m, e, pl.ds(r0, chunk)].astype(F32)
        sig = jax.nn.sigmoid(h1_f32)
        silu = h1_f32 * sig
        act = (silu * h3_f32).astype(BF16)
        grad_h1 = (grad_act * h3_f32 * sig * (1.0 + h1_f32 * (1.0 - sig))).astype(BF16)
        grad_h3 = (grad_act * silu).astype(BF16)
        rows = lax.dot_general(grad_h1, w1[e], nt, preferred_element_type=F32)
        rows = rows + lax.dot_general(grad_h3, w3[e], nt, preferred_element_type=F32)
        rows = rows.astype(BF16)
        blk = (c % per_exp) * (chunk // tokens)
        for h in range(2):
            out_rows(m)[h, e, pl.ds(blk, chunk // tokens)] = rows[:, h * half:(h + 1) * half].reshape(-1, tokens, half)
        h1[m, e, pl.ds(r0, chunk)] = grad_h1
        h3[m, e, pl.ds(r0, chunk)] = grad_h3
        act_v[m, e, pl.ds(r0, chunk)] = act

    def send_return(m):
        for which in range(2):
            for dx, dy in RETURN_ORDER:
                dst = (((chip_y + dy) % side) * side + (chip_x + dx) % side) * 2 + (core + which) % 2
                send_row(m, dst)
            if which == 0:
                send_row(m, me + 1 - 2 * core)

    def send_row(m, dst):
        pltpu.make_async_remote_copy(own_rows(m, dst), ret.at[m, me], ret_send, ret_recv.at[m],
                                     device_id={'ep': dst}, device_id_type=MESH).start()

    def combine(m):
        pad[...] = jnp.zeros_like(pad)
        pad[0:16] = route[me, m]
        key = jnp.transpose(pad[...])
        place = lax.broadcasted_iota(jnp.int32, (tokens, n_dev * rows_dev), 1).astype(F32)
        mat = jnp.zeros((tokens, n_dev * rows_dev), F32)
        for j in range(top_k):
            mat = jnp.where(place == key[:, j:j + 1], 1.0, mat)
        onehot[m] = mat.astype(BF16)
        ret[m, me] = own_rows(m, me)[...]
        pltpu.make_async_copy(ret.at[m, pl.ds(0, n_dev - 1)], ret.at[m, pl.ds(0, n_dev - 1)], ret_recv.at[m]).wait()
        for h in range(2):
            back = ret[m, :, h].reshape(n_dev * rows_dev, half)
            dx_ref[m, :, h * half:(h + 1) * half] = jnp.dot(onehot[m], back, preferred_element_type=F32).astype(BF16)

    pltpu.make_async_copy(route.at[pl.ds(0, n_route)], route.at[pl.ds(0, n_route)], route_recv).wait()
    items(0, 0, 8)
    items(1, 0, 2)
    items(0, 8, 16)
    items(1, 2, 8)

    def sent_part(m):
        return full.at[m, :, :, :, pl.ds(0, 7 * tokens // 8), :]

    def wait_dyd(m):
        part = dyd.at[m, :, pl.ds(0, (n_dev - 8) * capacity)]
        pltpu.make_async_copy(part, part, dyd_recv.at[m]).wait()

    for c in loads:
        c.wait()
    wait_dyd(0)

    def mixed(c, carry):
        compute(0, c)
        item(1, 8 + 2 * c)
        item(1, 9 + 2 * c)
        return carry

    lax.fori_loop(0, 2 * per_exp, mixed, 0)
    send_return(0)
    wait_dyd(1)
    pltpu.make_async_copy(sent_part(0), sent_part(0), full_send.at[0]).wait()
    lax.fori_loop(0, 2 * per_exp, lambda c, carry: (compute(1, c), carry)[1], 0)
    send_return(1)

    tile = d_ff // 2
    n_tile = d_model // tile
    rows_exp = n_dev * capacity

    def x_copy(i, m):
        col = pl.multiple_of((i % n_tile) * tile, tile)
        return pltpu.make_async_copy(x_hbm.at[m, i // n_tile, :, pl.ds(col, tile)],
                                     w1.at[i % 2, pl.ds(m * rows_exp, rows_exp), pl.ds(0, tile)], x_sem.at[i % 2, m])

    def dy_block(m):
        return w2.at[0, pl.ds((2 + m) * tokens, tokens), :]

    def y_copy(i):
        return pltpu.make_async_copy(yd_hbm.at[i // top_k, i % top_k],
                                     w2.at[0, pl.ds(pl.multiple_of((i % 2) * tokens, tokens), tokens), :], y_sem.at[i % 2])

    dy_loads = [pltpu.make_async_copy(dy_hbm.at[m], dy_block(m), load_sem.at[m]) for m in range(n_micro)]
    for m in range(n_micro):
        x_copy(0, m).start()
        dy_loads[m].start()
    y_copy(0).start()

    def weight_step(i, carry):
        @pl.when(i + 1 < 2 * n_tile)
        def _():
            for m in range(n_micro):
                x_copy(i + 1, m).start()

        for m in range(n_micro):
            x_copy(i, m).wait()
        e = i // n_tile
        col = pl.multiple_of((i % n_tile) * tile, tile)
        tn = (((0,), (0,)), ((), ()))
        x_blk = w1[i % 2, 0:n_micro * rows_exp, 0:tile]
        g1 = h1[:, e].reshape(n_micro * rows_exp, d_ff)
        g3 = h3[:, e].reshape(n_micro * rows_exp, d_ff)
        act = act_v[:, e].reshape(n_micro * rows_exp, d_ff)
        dy_blk = dyd[:, e, :, pl.ds(col, tile)].reshape(n_micro * rows_exp, tile)
        dw1_ref[e, pl.ds(col, tile), :] = lax.dot_general(x_blk, g1, tn, preferred_element_type=F32)
        dw3_ref[e, pl.ds(col, tile), :] = lax.dot_general(x_blk, g3, tn, preferred_element_type=F32)
        dw2_ref[e, :, pl.ds(col, tile)] = lax.dot_general(act, dy_blk, tn, preferred_element_type=F32)
        return carry

    lax.fori_loop(0, 2 * n_tile, weight_step, 0)
    for c in dy_loads:
        c.wait()
    lane = lax.broadcasted_iota(jnp.int32, (tokens, 128), 1)
    for m in range(n_micro):
        def gate_grad(j, total, m=m):
            i = m * top_k + j

            @pl.when(i + 1 < n_micro * top_k)
            def _():
                y_copy(i + 1).start()

            y_copy(i).wait()
            part = jnp.zeros((tokens, 128), F32)
            for c in range(0, d_model, 128):
                dy_blk = w2[0, (2 + m) * tokens:(3 + m) * tokens, c:c + 128].astype(F32)
                part = part + dy_blk * w2[0, pl.ds(pl.multiple_of((i % 2) * tokens, tokens), tokens), c:c + 128].astype(F32)
            return jnp.where(lane == j, jnp.sum(part, axis=1, keepdims=True), total)

        total = lax.fori_loop(0, top_k, gate_grad, jnp.zeros((tokens, 128), F32))
        dg_ref[:, m, :] = jnp.transpose(total)[0:top_k, :]
    for m in range(n_micro):
        combine(m)
    pltpu.make_async_copy(sent_part(1), sent_part(1), full_send.at[1]).wait()
    pltpu.make_async_copy(leaf, leaf, leaf_send).wait()
    pltpu.make_async_copy(sib, sib, sib_send).wait()
    pltpu.make_async_copy(route.at[pl.ds(0, n_route)], route.at[pl.ds(0, n_route)], route_send).wait()
    pltpu.make_async_copy(ret.at[:, pl.ds(0, n_dev - 1)], ret.at[:, pl.ds(0, n_dev - 1)], ret_send).wait()


def solution(mesh):
    n_dev = mesh.shape['ep']
    side = 1
    while 2 * side * side < n_dev:
        side += 1
    tok_spec = P(None, ('dp', 'ep'))
    w_spec = P('ep')
    grad_w_spec = P(('dp', 'ep'))

    def local_step(grad_out, expert_out, gate_vals, topk_idx, slot_idx, x_dispatch, h1_pre, h3_pre, w_gate, w_up, w_down):
        n_micro, tokens, top_k, d_model = expert_out.shape
        local_exp, _, d_ff = w_gate.shape
        rows = x_dispatch.shape[2]
        capacity = rows // n_dev
        half = d_model // 2
        hbm = pl.BlockSpec(memory_space=pl.ANY)
        by_choice = functools.partial(jnp.transpose, axes=(2, 0, 1))
        vmem = pl.BlockSpec(memory_space=pltpu.VMEM)
        dma = pltpu.SemaphoreType.DMA
        kernel = functools.partial(exchange_kernel, n_dev, side, n_micro, tokens, top_k, d_model, d_ff, capacity)
        ff_shape = (n_micro, local_exp, rows, d_ff)
        wide_shape = (n_micro, local_exp, rows, d_model)
        out_vmem = pltpu.VMEM
        grad_x, grad_gate, grad_w_gate, grad_w_up, grad_w_down = pl.pallas_call(
            kernel,
            name='exchange',
            out_shape=(
                out_vmem((n_micro, tokens, d_model), BF16),
                out_vmem((top_k, n_micro, tokens), F32),
                out_vmem(w_gate.shape, F32),
                out_vmem(w_up.shape, F32),
                out_vmem(w_down.shape, F32),
            ),
            in_specs=[hbm, hbm, vmem, vmem, vmem, hbm, hbm, hbm, hbm, hbm, hbm],
            out_specs=(vmem,) * 5,
            scratch_shapes=[
                pltpu.VMEM((n_micro, 2, 2, 4, tokens, half), BF16),
                pltpu.VMEM((n_micro, 2, 8, 2, local_exp, capacity, half), BF16),
                pltpu.VMEM((n_micro, 2, 8, local_exp, capacity, half), BF16),
                pltpu.VMEM(wide_shape, BF16),
                pltpu.VMEM((2, local_exp, rows // tokens, tokens, half), BF16),
                pltpu.VMEM((n_micro, n_dev, 2, local_exp, capacity, half), BF16),
                pltpu.VMEM((n_dev, n_micro, 16, tokens), F32),
                pltpu.VMEM((tokens, 128), F32),
                pltpu.VMEM(w_gate.shape, BF16),
                pltpu.VMEM(w_up.shape, BF16),
                pltpu.VMEM(w_down.shape, BF16),
                pltpu.VMEM(ff_shape, BF16),
                pltpu.VMEM(ff_shape, BF16),
                pltpu.VMEM(ff_shape, BF16),
                pltpu.VMEM((n_micro, tokens, n_dev * local_exp * capacity), BF16),
                dma((n_micro, 2, 8)),
                dma((n_micro,)),
                dma, dma,
                dma((n_micro,)),
                dma, dma, dma,
                dma((n_micro,)),
                dma((5,)),
                dma((2,)),
                dma((2, n_micro)),
            ],
            compiler_params=pltpu.CompilerParams(collective_id=0, has_side_effects=True, vmem_limit_bytes=VMEM_GRANT),
            cost_estimate=pl.CostEstimate(flops=10 ** 10, bytes_accessed=5 * 10 ** 7, transcendentals=0),
        )(grad_out, jnp.transpose(expert_out, (0, 2, 1, 3)), by_choice(gate_vals), by_choice(topk_idx), by_choice(slot_idx),
          x_dispatch, h1_pre, h3_pre, w_gate, w_up, w_down)
        grad_gate = jnp.transpose(grad_gate, (1, 2, 0))
        return grad_x, grad_gate, grad_w_gate, grad_w_up, grad_w_down

    in_specs = (tok_spec,) * 8 + (w_spec,) * 3
    out_specs = (tok_spec, tok_spec, grad_w_spec, grad_w_spec, grad_w_spec)
    return jax.shard_map(local_step, mesh=mesh, in_specs=in_specs, out_specs=out_specs, check_vma=False)
```

```python
import functools
import jax
import jax.numpy as jnp
from jax import lax
from jax.experimental import pallas as pl
from jax.experimental.pallas import tpu as pltpu
from jax.sharding import PartitionSpec as P

MESH = pl.DeviceIdType.MESH
BF16 = jnp.bfloat16
VMEM_GRANT = 67043328 - 13 * 2 ** 20
F32 = jnp.float32

def exchange_kernel(n_dev, side, n_micro, tokens, top_k, d_model, d_ff, capacity,
                    dy_hbm, yd_hbm, gate_ref, topk_ref, slot_ref, x_hbm, h1_hbm, h3_hbm, w1_hbm, w3_hbm, w2_hbm,
                    dx_ref, dg_ref, dw1_ref, dw3_ref, dw2_hbm,
                    full, leaf, sib, dyd, dxs, ret, land, d2, route, pad, w1, w3, w2, h1, h3, act_v, onehot,
                    full_recv, full_send, leaf_send, sib_send, dyd_recv, route_send, route_recv,
                    ret_send, ret_recv, turn_send, turn_recv, load_sem, y_sem, x_sem, d2_sem):
    me = lax.axis_index('ep')
    core = me % 2
    chip_x = (me // 2) % side
    chip_y = me // (2 * side)
    rows_dev = 2 * capacity
    half = d_model // 2

    def device(da, db, which):
        dx = da * (1 - core) + db * core
        dy = da * core + db * (1 - core)
        return (((chip_y + dy + 2 * side) % side) * side + (chip_x + dx + 2 * side) % side) * 2 + which

    def load_own(m, h):
        return pltpu.make_async_copy(dy_hbm.at[m, :, pl.ds(h * half, half)], full.at[m, h, 0, 0], full_recv.at[m, h, 0])

    for m in range(n_micro):
        for h in range(2):
            load_own(m, h).start()
    loads = [pltpu.make_async_copy(src, dst, load_sem.at[i]) for i, (src, dst) in enumerate(
        ((w2_hbm, w2), (h1_hbm, h1), (h3_hbm, h3), (w1_hbm, w1), (w3_hbm, w3)))]

    barrier = pltpu.get_barrier_semaphore()

    def greet(k, carry):
        pl.semaphore_signal(barrier, inc=1, device_id={'ep': (me + k) % n_dev}, device_id_type=MESH)
        return carry

    lax.fori_loop(1, n_dev, greet, 0)
    for c in loads:
        c.start()

    for m in range(n_micro):
        slot = slot_ref[:, m, :]
        key = jnp.where(slot >= 0, topk_ref[:, m, :] * capacity + slot, -1)
        route[me, m] = jnp.zeros((16, tokens), F32)
        route[me, m, 0:top_k] = key.astype(F32)
        route[me, m, 8:8 + top_k] = gate_ref[:, m, :]
    pl.semaphore_wait(barrier, n_dev - 1)

    def send_route(da, db):
        pltpu.make_async_remote_copy(route.at[me], route.at[me], route_send, route_recv,
                                     device_id={'ep': device(da, db, core)}, device_id_type=MESH).start()

    n_route = 0
    for da, db in ((1, 0), (side - 1, 0), (2, 0), (0, 1), (0, side - 1), (1, 1), (1, side - 1), (side - 1, 1),
                   (side - 1, side - 1), (2, 1), (2, side - 1)):
        send_route(da, db)
        n_route += 1

    def send_full(m, h, ev, da, db, slot):
        pltpu.make_async_remote_copy(full.at[m, h, ev // 4, ev % 4], full.at[m, h, slot // 4, slot % 4],
                                     full_send.at[m], full_recv.at[m, h, slot],
                                     device_id={'ep': device(da, db, core)}, device_id_type=MESH).start()

    def forward(m, h, ev):
        s = 1 - 2 * h
        k = ev % 4
        lvl = ev // 4
        tok = full.at[m, h, lvl, k]
        pltpu.make_async_copy(tok, tok, full_recv.at[m, h, ev]).wait()

        @pl.when(ev == 0)
        def _():
            send_full(m, h, ev, s, 0, 1)
            send_full(m, h, ev, -s, 0, 2)

        @pl.when(ev == 1)
        def _():
            send_full(m, h, ev, s, 0, 3)

        @pl.when(ev < 4)
        def _():
            send_full(m, h, ev, 0, s, 4 + ev)

    def pack(m, h, ev):
        s = 1 - 2 * h
        k = ev % 4
        lvl = ev // 4
        tok = full.at[m, h, lvl, k]
        da = (k % 2) * (1 - k // 2) * (-s) + (k // 2) * (1 - k % 2) * s + (k // 2) * (k % 2) * 2
        home = device(da, -s * lvl, core)
        leaf_chip = device(0, s * (2 * lvl - 1), 0)
        row = lax.broadcasted_iota(jnp.int32, (4 * rows_dev, tokens), 0)
        block = row // rows_dev
        inner = row - block * rows_dev
        dev = jnp.where(block == 0, me, jnp.where(block == 1, me + 1 - 2 * core,
                                                  jnp.where(block == 2, leaf_chip, leaf_chip + 1)))
        want = (dev * rows_dev + inner).astype(F32)
        table = route[home, m]
        pick = jnp.zeros((4 * rows_dev, tokens), F32)
        gate = jnp.zeros((4 * rows_dev, tokens), F32)
        for j in range(top_k):
            hit = want == table[j:j + 1, :]
            pick = jnp.where(hit, 1.0, pick)
            gate = jnp.where(hit, table[8 + j:9 + j, :], gate)
        gate = jnp.sum(gate, axis=1, keepdims=True)
        rows = jnp.dot(pick.astype(BF16), tok[...], preferred_element_type=F32)
        rows = (rows * gate).astype(BF16)
        leaf[m, h, ev] = rows[2 * rows_dev:].reshape(2, 2, capacity, half)
        sib[m, h, ev] = rows[rows_dev:2 * rows_dev].reshape(2, capacity, half)
        row0 = pl.multiple_of(home * capacity, capacity)
        col0 = pl.multiple_of(h * half, half)
        dyd[m, :, pl.ds(row0, capacity), pl.ds(col0, half)] = rows[:rows_dev].reshape(2, capacity, half)
        target = dyd.at[m, :, pl.ds(row0, capacity), pl.ds(col0, half)]
        for c in range(2):
            pltpu.make_async_remote_copy(leaf.at[m, h, ev, c], target, leaf_send, dyd_recv.at[m],
                                         device_id={'ep': leaf_chip + c}, device_id_type=MESH).start()
        pltpu.make_async_remote_copy(sib.at[m, h, ev], target, sib_send, dyd_recv.at[m],
                                     device_id={'ep': me + 1 - 2 * core}, device_id_type=MESH).start()

    def item(m, ev):
        for h in range(2):
            forward(m, h, ev)
        for h in range(2):
            pack(m, h, ev)

    def items(m, lo, hi):
        lax.fori_loop(lo, hi, lambda ev, c: (item(m, ev), c)[1], 0)

    chunk = 256
    per_exp = (n_dev * capacity) // chunk

    def out_rows(m):
        return dxs if m == 0 else full.at[0]

    def own_rows(m, dst):
        row0 = pl.multiple_of((dst % (tokens // capacity)) * capacity, capacity)
        return out_rows(m).at[:, :, dst // (tokens // capacity), pl.ds(row0, capacity), :]

    def compute(m, c):
        e = c // per_exp
        r0 = pl.multiple_of((c % per_exp) * chunk, chunk)
        nt = (((1,), (1,)), ((), ()))
        grad_act = lax.dot_general(dyd[m, e, pl.ds(r0, chunk)], w2[e], nt, preferred_element_type=F32)
        grad_act = grad_act.astype(BF16).astype(F32)
        h1_f32 = h1[m, e, pl.ds(r0, chunk)].astype(F32)
        h3_f32 = h3[m, e, pl.ds(r0, chunk)].astype(F32)
        sig = jax.nn.sigmoid(h1_f32)
        silu = h1_f32 * sig
        act = (silu * h3_f32).astype(BF16)
        grad_h1 = (grad_act * h3_f32 * sig * (1.0 + h1_f32 * (1.0 - sig))).astype(BF16)
        grad_h3 = (grad_act * silu).astype(BF16)
        rows = lax.dot_general(grad_h1, w1[e], nt, preferred_element_type=F32)
        rows = rows + lax.dot_general(grad_h3, w3[e], nt, preferred_element_type=F32)
        rows = rows.astype(BF16)
        blk = (c % per_exp) * (chunk // tokens)
        for h in range(2):
            out_rows(m)[h, e, pl.ds(blk, chunk // tokens)] = rows[:, h * half:(h + 1) * half].reshape(-1, tokens, half)
        h1[m, e, pl.ds(r0, chunk)] = grad_h1
        h3[m, e, pl.ds(r0, chunk)] = grad_h3
        act_v[m, e, pl.ds(r0, chunk)] = act

    pair_rows = 2 * capacity
    n_turn = side * (side - 1)

    def send_home(src, m, owner, dst):
        pltpu.make_async_remote_copy(src, ret.at[m, owner], ret_send.at[m], ret_recv.at[m],
                                     device_id={'ep': dst}, device_id_type=MESH).start()

    def send_return(m):
        def turn(i, carry):
            da, db = (i // (side - 1) + 1) % side, i % (side - 1) + 1
            chip = device(da, db, 0) // 2
            per_blk = tokens // pair_rows
            row0 = pl.multiple_of((chip % per_blk) * pair_rows, pair_rows)
            pltpu.make_async_remote_copy(out_rows(m).at[:, :, chip // per_blk, pl.ds(row0, pair_rows), :], land.at[m, i],
                                         turn_send.at[m], turn_recv.at[m, i],
                                         device_id={'ep': device(0, db, core)}, device_id_type=MESH).start()
            return carry

        def straight(i, carry):
            dst = device(i // 2, 0, i % 2)
            send_home(own_rows(m, dst), m, me, dst)
            return carry

        lax.fori_loop(2, 2 * side, straight, 0)
        lax.fori_loop(0, n_turn, turn, 0)
        send_home(own_rows(m, me + 1 - 2 * core), m, me, me + 1 - 2 * core)

    def relay(m, i):
        da, db = (i // (side - 1) + 1) % side, i % (side - 1) + 1
        pltpu.make_async_copy(land.at[m, i], land.at[m, i], turn_recv.at[m, i]).wait()
        owner = device(0, -db, core)

        def part(which):
            return land.at[m, i, :, :, pl.ds(pl.multiple_of(which * capacity, capacity), capacity), :]

        @pl.when(da != 0)
        def _():
            for which in range(2):
                send_home(part(which), m, owner, device(da, 0, which))

        @pl.when(da == 0)
        def _():
            send_home(part(1 - core), m, owner, me + 1 - 2 * core)
            ret[m, owner] = part(core)[...]

    def relays(m, lo, hi):
        lax.fori_loop(lo, hi, lambda i, c: (relay(m, i), c)[1], 0)

    n_home = n_dev - side

    def combine(m):
        pad[...] = jnp.zeros_like(pad)
        pad[0:16] = route[me, m]
        key = jnp.transpose(pad[...])
        place = lax.broadcasted_iota(jnp.int32, (tokens, n_dev * rows_dev), 1).astype(F32)
        mat = jnp.zeros((tokens, n_dev * rows_dev), F32)
        for j in range(top_k):
            mat = jnp.where(place == key[:, j:j + 1], 1.0, mat)
        onehot[m] = mat.astype(BF16)
        ret[m, me] = own_rows(m, me)[...]
        pltpu.make_async_copy(ret.at[m, pl.ds(0, n_home)], ret.at[m, pl.ds(0, n_home)], ret_recv.at[m]).wait()
        for h in range(2):
            back = ret[m, :, h].reshape(n_dev * rows_dev, half)
            dx_ref[m, :, h * half:(h + 1) * half] = jnp.dot(onehot[m], back, preferred_element_type=F32).astype(BF16)

    pltpu.make_async_copy(route.at[pl.ds(0, n_route)], route.at[pl.ds(0, n_route)], route_recv).wait()
    items(0, 0, 4)
    items(1, 0, 1)
    items(0, 4, 8)
    items(1, 1, 4)

    def sent_part(m):
        return full.at[m, :, :, :, pl.ds(0, 7 * tokens // 8), :]

    def wait_dyd(m):
        part = dyd.at[m, :, pl.ds(0, (n_dev - 8) * capacity)]
        pltpu.make_async_copy(part, part, dyd_recv.at[m]).wait()

    for c in loads:
        c.wait()
    wait_dyd(0)

    def mixed(c, carry):
        compute(0, c)
        item(1, 4 + c)
        return carry

    lax.fori_loop(0, 2 * per_exp, mixed, 0)
    send_return(0)
    wait_dyd(1)
    pltpu.make_async_copy(sent_part(0), sent_part(0), full_send.at[0]).wait()
    lax.fori_loop(0, 2 * per_exp, lambda c, carry: (compute(1, c), carry)[1], 0)
    send_return(1)

    tile = d_ff // 2
    n_tile = d_model // tile
    rows_exp = n_dev * capacity

    def x_copy(i, m):
        col = pl.multiple_of((i % n_tile) * tile, tile)
        return pltpu.make_async_copy(x_hbm.at[m, i // n_tile, :, pl.ds(col, tile)],
                                     w1.at[i % 2, pl.ds(m * rows_exp, rows_exp), pl.ds(0, tile)], x_sem.at[i % 2, m])

    def dy_block(m):
        return w2.at[0, pl.ds((2 + m) * tokens, tokens), :]

    def y_copy(i):
        return pltpu.make_async_copy(yd_hbm.at[i // top_k, i % top_k],
                                     w2.at[0, pl.ds(pl.multiple_of((i % 2) * tokens, tokens), tokens), :], y_sem.at[i % 2])

    dy_loads = [pltpu.make_async_copy(dy_hbm.at[m], dy_block(m), load_sem.at[m]) for m in range(n_micro)]
    for m in range(n_micro):
        x_copy(0, m).start()
        dy_loads[m].start()
    y_copy(0).start()

    done0 = 0

    def d2_copy(i):
        col = pl.multiple_of((i % n_tile) * tile, tile)
        return pltpu.make_async_copy(d2.at[i % 2], dw2_hbm.at[i // n_tile, :, pl.ds(col, tile)], d2_sem.at[i % 2])

    def weight_step(i, carry):
        @pl.when(i + 1 < 2 * n_tile)
        def _():
            for m in range(n_micro):
                x_copy(i + 1, m).start()

        for m in range(n_micro):
            x_copy(i, m).wait()
        e = i // n_tile
        col = pl.multiple_of((i % n_tile) * tile, tile)
        tn = (((0,), (0,)), ((), ()))
        x_blk = w1[i % 2, 0:n_micro * rows_exp, 0:tile]
        g1 = h1[:, e].reshape(n_micro * rows_exp, d_ff)
        g3 = h3[:, e].reshape(n_micro * rows_exp, d_ff)
        act = act_v[:, e].reshape(n_micro * rows_exp, d_ff)
        dy_blk = dyd[:, e, :, pl.ds(col, tile)].reshape(n_micro * rows_exp, tile)
        dw1_ref[e, pl.ds(col, tile), :] = lax.dot_general(x_blk, g1, tn, preferred_element_type=F32)
        dw3_ref[e, pl.ds(col, tile), :] = lax.dot_general(x_blk, g3, tn, preferred_element_type=F32)
        @pl.when(i >= 2)
        def _():
            d2_copy(i - 2).wait()

        d2[i % 2] = lax.dot_general(act, dy_blk, tn, preferred_element_type=F32)
        d2_copy(i).start()

        @pl.when(i + done0 < n_turn)
        def _():
            relay(0, i + done0)

        @pl.when(i + done0 >= n_turn)
        def _():
            relay(1, i + done0 - n_turn)

        return carry

    lax.fori_loop(0, 2 * n_tile, weight_step, 0)
    for i in (2 * n_tile - 2, 2 * n_tile - 1):
        d2_copy(i).wait()
    done1 = 2 * n_tile + done0 - n_turn
    for c in dy_loads:
        c.wait()
    lane = lax.broadcasted_iota(jnp.int32, (tokens, 128), 1)
    for m in range(n_micro):
        def gate_grad(j, total, m=m):
            i = m * top_k + j

            @pl.when(i + 1 < n_micro * top_k)
            def _():
                y_copy(i + 1).start()

            y_copy(i).wait()
            part = jnp.zeros((tokens, 128), F32)
            for c in range(0, d_model, 128):
                dy_blk = w2[0, (2 + m) * tokens:(3 + m) * tokens, c:c + 128].astype(F32)
                part = part + dy_blk * w2[0, pl.ds(pl.multiple_of((i % 2) * tokens, tokens), tokens), c:c + 128].astype(F32)
            @pl.when(i + done1 < n_turn - 2)
            def _():
                relay(1, i + done1)

            return jnp.where(lane == j, jnp.sum(part, axis=1, keepdims=True), total)

        total = lax.fori_loop(0, top_k, gate_grad, jnp.zeros((tokens, 128), F32))
        dg_ref[:, m, :] = jnp.transpose(total)[0:top_k, :]
    combine(0)
    relays(1, n_turn - 2, n_turn)
    combine(1)
    pltpu.make_async_copy(sent_part(1), sent_part(1), full_send.at[1]).wait()
    pltpu.make_async_copy(leaf, leaf, leaf_send).wait()
    pltpu.make_async_copy(sib, sib, sib_send).wait()
    pltpu.make_async_copy(route.at[pl.ds(0, n_route)], route.at[pl.ds(0, n_route)], route_send).wait()
    for m in range(n_micro):
        pltpu.make_async_copy(ret.at[m, pl.ds(0, n_home)], ret.at[m, pl.ds(0, n_home)], ret_send.at[m]).wait()
        pltpu.make_async_copy(land.at[m], land.at[m], turn_send.at[m]).wait()


def solution(mesh):
    n_dev = mesh.shape['ep']
    side = 1
    while 2 * side * side < n_dev:
        side += 1
    tok_spec = P(None, ('dp', 'ep'))
    w_spec = P('ep')
    grad_w_spec = P(('dp', 'ep'))

    def local_step(grad_out, expert_out, gate_vals, topk_idx, slot_idx, x_dispatch, h1_pre, h3_pre, w_gate, w_up, w_down):
        n_micro, tokens, top_k, d_model = expert_out.shape
        local_exp, _, d_ff = w_gate.shape
        rows = x_dispatch.shape[2]
        capacity = rows // n_dev
        half = d_model // 2
        hbm = pl.BlockSpec(memory_space=pl.ANY)
        by_choice = functools.partial(jnp.transpose, axes=(2, 0, 1))
        vmem = pl.BlockSpec(memory_space=pltpu.VMEM)
        dma = pltpu.SemaphoreType.DMA
        kernel = functools.partial(exchange_kernel, n_dev, side, n_micro, tokens, top_k, d_model, d_ff, capacity)
        ff_shape = (n_micro, local_exp, rows, d_ff)
        wide_shape = (n_micro, local_exp, rows, d_model)
        out_vmem = pltpu.VMEM
        grad_x, grad_gate, grad_w_gate, grad_w_up, grad_w_down = pl.pallas_call(
            kernel,
            name='exchange',
            out_shape=(
                out_vmem((n_micro, tokens, d_model), BF16),
                out_vmem((top_k, n_micro, tokens), F32),
                out_vmem(w_gate.shape, F32),
                out_vmem(w_up.shape, F32),
                pltpu.HBM(w_down.shape, F32),
            ),
            in_specs=[hbm, hbm, vmem, vmem, vmem, hbm, hbm, hbm, hbm, hbm, hbm],
            out_specs=(vmem,) * 4 + (hbm,),
            scratch_shapes=[
                pltpu.VMEM((n_micro, 2, 2, 4, tokens, half), BF16),
                pltpu.VMEM((n_micro, 2, 8, 2, local_exp, capacity, half), BF16),
                pltpu.VMEM((n_micro, 2, 8, local_exp, capacity, half), BF16),
                pltpu.VMEM(wide_shape, BF16),
                pltpu.VMEM((2, local_exp, rows // tokens, tokens, half), BF16),
                pltpu.VMEM((n_micro, n_dev, 2, local_exp, capacity, half), BF16),
                pltpu.VMEM((n_micro, side * (side - 1), 2, local_exp, 2 * capacity, half), BF16),
                pltpu.VMEM((2, d_ff, d_ff // 2), F32),
                pltpu.VMEM((n_dev, n_micro, 16, tokens), F32),
                pltpu.VMEM((tokens, 128), F32),
                pltpu.VMEM(w_gate.shape, BF16),
                pltpu.VMEM(w_up.shape, BF16),
                pltpu.VMEM(w_down.shape, BF16),
                pltpu.VMEM(ff_shape, BF16),
                pltpu.VMEM(ff_shape, BF16),
                pltpu.VMEM(ff_shape, BF16),
                pltpu.VMEM((n_micro, tokens, n_dev * local_exp * capacity), BF16),
                dma((n_micro, 2, 8)),
                dma((n_micro,)),
                dma, dma,
                dma((n_micro,)),
                dma, dma,
                dma((n_micro,)),
                dma((n_micro,)),
                dma((n_micro,)),
                dma((n_micro, side * (side - 1))),
                dma((5,)),
                dma((2,)),
                dma((2, n_micro)),
                dma((2,)),
            ],
            compiler_params=pltpu.CompilerParams(collective_id=0, has_side_effects=True, vmem_limit_bytes=VMEM_GRANT),
            cost_estimate=pl.CostEstimate(flops=10 ** 10, bytes_accessed=5 * 10 ** 7, transcendentals=0),
        )(grad_out, jnp.transpose(expert_out, (0, 2, 1, 3)), by_choice(gate_vals), by_choice(topk_idx), by_choice(slot_idx),
          x_dispatch, h1_pre, h3_pre, w_gate, w_up, w_down)
        grad_gate = jnp.transpose(grad_gate, (1, 2, 0))
        return grad_x, grad_gate, grad_w_gate, grad_w_up, grad_w_down

    in_specs = (tok_spec,) * 8 + (w_spec,) * 3
    out_specs = (tok_spec, tok_spec, grad_w_spec, grad_w_spec, grad_w_spec)
    return jax.shard_map(local_step, mesh=mesh, in_specs=in_specs, out_specs=out_specs, check_vma=False)
```

```python
import functools
import jax
import jax.numpy as jnp
from jax import lax
from jax.experimental import pallas as pl
from jax.experimental.pallas import tpu as pltpu
from jax.sharding import PartitionSpec as P

MESH = pl.DeviceIdType.MESH
BF16 = jnp.bfloat16
VMEM_GRANT = 67043328 - 13 * 2 ** 20 + 160 * 2 ** 10
F32 = jnp.float32
NODES = ((0, 0), (1, 0), (0, 1), (2, 0), (0, 2), (2, 3))
EDGES = ((0, (1, 0), 1), (0, (0, 1), 2), (1, (1, 0), 3), (2, (0, 1), 4), (3, (0, -1), 5))
LEAVES = (((-1, 0), (0, -1)), ((0, 1), (0, -1)), ((-1, 0), (-1, 0)), ((0, 1), (0, 1)), ((1, 0), (-1, 0)), ((0, -1), (1, 0)))


def exchange_kernel(n_dev, side, n_micro, tokens, top_k, d_model, d_ff, capacity,
                    dy_hbm, yd_hbm, gate_ref, topk_ref, slot_ref, x_hbm, h1_hbm, h3_hbm, w1_hbm, w3_hbm, w2_hbm,
                    dx_ref, dg_ref, dw1_ref, dw3_ref, dw2_hbm,
                    full, leaf, sib, dyd, dxs, ret, land, d2, route, pad, w1, w3, w2, h1, h3, act_v, onehot,
                    full_recv, full_send, leaf_send, sib_send, dyd_recv, route_send, route_recv,
                    ret_send, ret_recv, turn_send, turn_recv, load_sem, y_sem, x_sem, d2_sem):
    me = lax.axis_index('ep')
    core = me % 2
    chip_x = (me // 2) % side
    chip_y = me // (2 * side)
    rows_dev = 2 * capacity
    half = d_model // 2

    def device(da, db, which):
        dx = da * (1 - core) + db * core
        dy = da * core + db * (1 - core)
        return (((chip_y + dy + 2 * side) % side) * side + (chip_x + dx + 2 * side) % side) * 2 + which

    def load_own(m, h):
        return pltpu.make_async_copy(dy_hbm.at[m, :, pl.ds(h * half, half)], full.at[m, h, 0, 0], full_recv.at[m, h, 0])

    for m in range(n_micro):
        for h in range(2):
            load_own(m, h).start()
    loads = [pltpu.make_async_copy(src, dst, load_sem.at[i]) for i, (src, dst) in enumerate(
        ((w2_hbm, w2), (h1_hbm, h1), (h3_hbm, h3), (w1_hbm, w1), (w3_hbm, w3)))]

    barrier = pltpu.get_barrier_semaphore()

    def greet(k, carry):
        pl.semaphore_signal(barrier, inc=1, device_id={'ep': (me + k) % n_dev}, device_id_type=MESH)
        return carry

    lax.fori_loop(1, n_dev, greet, 0)
    for c in loads:
        c.start()

    for m in range(n_micro):
        slot = slot_ref[:, m, :]
        key = jnp.where(slot >= 0, topk_ref[:, m, :] * capacity + slot, -1)
        route[me, m] = jnp.zeros((16, tokens), F32)
        route[me, m, 0:top_k] = key.astype(F32)
        route[me, m, 8:8 + top_k] = gate_ref[:, m, :]
    pl.semaphore_wait(barrier, n_dev - 1)

    def send_route(da, db):
        pltpu.make_async_remote_copy(route.at[me], route.at[me], route_send, route_recv,
                                     device_id={'ep': device(da, db, core)}, device_id_type=MESH).start()

    n_route = 0
    for da, db in sorted({(q * a % side, q * b % side) for a, b in NODES[1:] for q in (1, -1)}):
        send_route(da, db)
        n_route += 1

    def send_full(m, h, ev, da, db, slot):
        pltpu.make_async_remote_copy(full.at[m, h, ev // 4, ev % 4], full.at[m, h, slot // 4, slot % 4],
                                     full_send.at[m], full_recv.at[m, h, slot],
                                     device_id={'ep': device(da, db, core)}, device_id_type=MESH).start()

    def forward(m, h, ev):
        s = 1 - 2 * h
        tok = full.at[m, h, ev // 4, ev % 4]
        pltpu.make_async_copy(tok, tok, full_recv.at[m, h, ev]).wait()
        for src, (da, db), slot in EDGES:
            @pl.when(ev == src)
            def _(da=da, db=db, slot=slot):
                send_full(m, h, ev, s * da, s * db, slot)

    def by_event(ev, values):
        out = values[0]
        for i, v in enumerate(values[1:]):
            out = jnp.where(ev == i + 1, v, out)
        return out

    def pack(m, h, ev):
        s = 1 - 2 * h
        tok = full.at[m, h, ev // 4, ev % 4]
        home = device(-s * by_event(ev, [p[0] for p in NODES]), -s * by_event(ev, [p[1] for p in NODES]), core)
        leaf_chip = [device(s * by_event(ev, [p[i][0] for p in LEAVES]), s * by_event(ev, [p[i][1] for p in LEAVES]), 0)
                     for i in range(2)]
        row = lax.broadcasted_iota(jnp.int32, (6 * rows_dev, tokens), 0)
        block = row // rows_dev
        inner = row - block * rows_dev
        dev = jnp.where(block < 4, leaf_chip[0] + block - 2, leaf_chip[1] + block - 4)
        dev = jnp.where(block == 0, me, jnp.where(block == 1, me + 1 - 2 * core, dev))
        want = (dev * rows_dev + inner).astype(F32)
        table = route[home, m]
        pick = jnp.zeros((6 * rows_dev, tokens), F32)
        gate = jnp.zeros((6 * rows_dev, tokens), F32)
        for j in range(top_k):
            hit = want == table[j:j + 1, :]
            pick = jnp.where(hit, 1.0, pick)
            gate = jnp.where(hit, table[8 + j:9 + j, :], gate)
        gate = jnp.sum(gate, axis=1, keepdims=True)
        rows = jnp.dot(pick.astype(BF16), tok[...], preferred_element_type=F32)
        rows = (rows * gate).astype(BF16)
        leaf[m, h, ev] = rows[2 * rows_dev:].reshape(2, 2, 2, capacity, half)
        sib[m, h, ev] = rows[rows_dev:2 * rows_dev].reshape(2, capacity, half)
        row0 = pl.multiple_of(home * capacity, capacity)
        col0 = pl.multiple_of(h * half, half)
        dyd[m, :, pl.ds(row0, capacity), pl.ds(col0, half)] = rows[:rows_dev].reshape(2, capacity, half)
        target = dyd.at[m, :, pl.ds(row0, capacity), pl.ds(col0, half)]

        def send_leaf(i):
            for c in range(2):
                pltpu.make_async_remote_copy(leaf.at[m, h, ev, i, c], target, leaf_send, dyd_recv.at[m],
                                             device_id={'ep': leaf_chip[i] + c}, device_id_type=MESH).start()

        send_leaf(0)

        @pl.when(by_event(ev, [int(len(set(p)) == 2) for p in LEAVES]) == 1)
        def _():
            send_leaf(1)

        pltpu.make_async_remote_copy(sib.at[m, h, ev], target, sib_send, dyd_recv.at[m],
                                     device_id={'ep': me + 1 - 2 * core}, device_id_type=MESH).start()

    def item(m, ev):
        for h in range(2):
            forward(m, h, ev)
        for h in range(2):
            pack(m, h, ev)

    def items(m, lo, hi):
        lax.fori_loop(lo, hi, lambda ev, c: (item(m, ev), c)[1], 0)

    chunk = 256
    per_exp = (n_dev * capacity) // chunk

    def out_rows(m):
        return dxs if m == 0 else full.at[0]

    def own_rows(m, dst):
        row0 = pl.multiple_of((dst % (tokens // capacity)) * capacity, capacity)
        return out_rows(m).at[:, :, dst // (tokens // capacity), pl.ds(row0, capacity), :]

    def compute(m, c):
        e = c // per_exp
        r0 = pl.multiple_of((c % per_exp) * chunk, chunk)
        nt = (((1,), (1,)), ((), ()))
        grad_act = lax.dot_general(dyd[m, e, pl.ds(r0, chunk)], w2[e], nt, preferred_element_type=F32)
        grad_act = grad_act.astype(BF16).astype(F32)
        h1_f32 = h1[m, e, pl.ds(r0, chunk)].astype(F32)
        h3_f32 = h3[m, e, pl.ds(r0, chunk)].astype(F32)
        sig = jax.nn.sigmoid(h1_f32)
        silu = h1_f32 * sig
        act = (silu * h3_f32).astype(BF16)
        grad_h1 = (grad_act * h3_f32 * sig * (1.0 + h1_f32 * (1.0 - sig))).astype(BF16)
        grad_h3 = (grad_act * silu).astype(BF16)
        rows = lax.dot_general(grad_h1, w1[e], nt, preferred_element_type=F32)
        rows = rows + lax.dot_general(grad_h3, w3[e], nt, preferred_element_type=F32)
        rows = rows.astype(BF16)
        blk = (c % per_exp) * (chunk // tokens)
        for h in range(2):
            out_rows(m)[h, e, pl.ds(blk, chunk // tokens)] = rows[:, h * half:(h + 1) * half].reshape(-1, tokens, half)
        h1[m, e, pl.ds(r0, chunk)] = grad_h1
        h3[m, e, pl.ds(r0, chunk)] = grad_h3
        act_v[m, e, pl.ds(r0, chunk)] = act

    pair_rows = 2 * capacity
    n_turn = side * (side - 1)

    def send_home(src, m, owner, dst):
        pltpu.make_async_remote_copy(src, ret.at[m, owner], ret_send.at[m], ret_recv.at[m],
                                     device_id={'ep': dst}, device_id_type=MESH).start()

    def send_return(m):
        def turn(i, carry):
            da, db = (i // (side - 1) + 1) % side, i % (side - 1) + 1
            chip = device(da, db, 0) // 2
            per_blk = tokens // pair_rows
            row0 = pl.multiple_of((chip % per_blk) * pair_rows, pair_rows)
            pltpu.make_async_remote_copy(out_rows(m).at[:, :, chip // per_blk, pl.ds(row0, pair_rows), :], land.at[m, i],
                                         turn_send.at[m], turn_recv.at[m, i],
                                         device_id={'ep': device(0, db, core)}, device_id_type=MESH).start()
            return carry

        def straight(i, carry):
            dst = device(i // 2, 0, i % 2)
            send_home(own_rows(m, dst), m, me, dst)
            return carry

        lax.fori_loop(2, 2 * side, straight, 0)
        lax.fori_loop(0, n_turn, turn, 0)
        send_home(own_rows(m, me + 1 - 2 * core), m, me, me + 1 - 2 * core)

    def relay(m, i):
        da, db = (i // (side - 1) + 1) % side, i % (side - 1) + 1
        pltpu.make_async_copy(land.at[m, i], land.at[m, i], turn_recv.at[m, i]).wait()
        owner = device(0, -db, core)

        def part(which):
            return land.at[m, i, :, :, pl.ds(pl.multiple_of(which * capacity, capacity), capacity), :]

        @pl.when(da != 0)
        def _():
            for which in range(2):
                send_home(part(which), m, owner, device(da, 0, which))

        @pl.when(da == 0)
        def _():
            send_home(part(1 - core), m, owner, me + 1 - 2 * core)
            ret[m, owner] = part(core)[...]

    def relays(m, lo, hi):
        lax.fori_loop(lo, hi, lambda i, c: (relay(m, i), c)[1], 0)

    n_home = n_dev - side

    def combine(m):
        pad[...] = jnp.zeros_like(pad)
        pad[0:16] = route[me, m]
        key = jnp.transpose(pad[...])
        place = lax.broadcasted_iota(jnp.int32, (tokens, n_dev * rows_dev), 1).astype(F32)
        mat = jnp.zeros((tokens, n_dev * rows_dev), F32)
        for j in range(top_k):
            mat = jnp.where(place == key[:, j:j + 1], 1.0, mat)
        onehot[...] = mat.astype(BF16)
        ret[m, me] = own_rows(m, me)[...]
        pltpu.make_async_copy(ret.at[m, pl.ds(0, n_home)], ret.at[m, pl.ds(0, n_home)], ret_recv.at[m]).wait()
        for h in range(2):
            for c in range(0, half, 256):
                back = ret[m, :, h, :, :, c:c + 256].reshape(n_dev * rows_dev, 256)
                dx_ref[m, :, h * half + c:h * half + c + 256] = jnp.dot(
                    onehot[...], back, preferred_element_type=F32).astype(BF16)

    pltpu.make_async_copy(route.at[pl.ds(0, n_route)], route.at[pl.ds(0, n_route)], route_recv).wait()
    items(0, 0, 3)
    items(1, 0, 1)
    items(0, 3, 6)
    items(1, 1, 2)

    def sent_part(m):
        return full.at[m, :, :, :, pl.ds(0, len(EDGES) * tokens // 8), :]

    def wait_dyd(m):
        part = dyd.at[m, :, pl.ds(0, (n_dev - len(NODES)) * capacity)]
        pltpu.make_async_copy(part, part, dyd_recv.at[m]).wait()

    for c in loads:
        c.wait()
    wait_dyd(0)

    def mixed(c, carry):
        compute(0, c)
        item(1, 2 + c)
        return carry

    lax.fori_loop(0, 2 * per_exp, mixed, 0)
    send_return(0)
    wait_dyd(1)
    pltpu.make_async_copy(sent_part(0), sent_part(0), full_send.at[0]).wait()
    lax.fori_loop(0, 2 * per_exp, lambda c, carry: (compute(1, c), carry)[1], 0)
    send_return(1)

    tile = d_ff // 2
    n_tile = d_model // tile
    rows_exp = n_dev * capacity

    def x_copy(i, m):
        col = pl.multiple_of((i % n_tile) * tile, tile)
        return pltpu.make_async_copy(x_hbm.at[m, i // n_tile, :, pl.ds(col, tile)],
                                     w1.at[i % 2, pl.ds(m * rows_exp, rows_exp), pl.ds(0, tile)], x_sem.at[i % 2, m])

    def dy_block(m):
        return w2.at[0, pl.ds((2 + m) * tokens, tokens), :]

    def y_copy(i):
        return pltpu.make_async_copy(yd_hbm.at[i // top_k, i % top_k],
                                     w2.at[0, pl.ds(pl.multiple_of((i % 2) * tokens, tokens), tokens), :], y_sem.at[i % 2])

    dy_loads = [pltpu.make_async_copy(dy_hbm.at[m], dy_block(m), load_sem.at[m]) for m in range(n_micro)]
    for m in range(n_micro):
        x_copy(0, m).start()
        dy_loads[m].start()
    y_copy(0).start()

    done0 = 0

    def d2_copy(i):
        col = pl.multiple_of((i % n_tile) * tile, tile)
        return pltpu.make_async_copy(d2.at[0], dw2_hbm.at[i // n_tile, :, pl.ds(col, tile)], d2_sem.at[0])

    def weight_step(i, carry):
        @pl.when(i + 1 < 2 * n_tile)
        def _():
            for m in range(n_micro):
                x_copy(i + 1, m).start()

        for m in range(n_micro):
            x_copy(i, m).wait()
        e = i // n_tile
        col = pl.multiple_of((i % n_tile) * tile, tile)
        tn = (((0,), (0,)), ((), ()))
        x_blk = w1[i % 2, 0:n_micro * rows_exp, 0:tile]
        g1 = h1[:, e].reshape(n_micro * rows_exp, d_ff)
        g3 = h3[:, e].reshape(n_micro * rows_exp, d_ff)
        act = act_v[:, e].reshape(n_micro * rows_exp, d_ff)
        dy_blk = dyd[:, e, :, pl.ds(col, tile)].reshape(n_micro * rows_exp, tile)
        dw1_ref[e, pl.ds(col, tile), :] = lax.dot_general(x_blk, g1, tn, preferred_element_type=F32)
        dw3_ref[e, pl.ds(col, tile), :] = lax.dot_general(x_blk, g3, tn, preferred_element_type=F32)
        @pl.when(i >= 1)
        def _():
            d2_copy(i - 1).wait()

        d2[0] = lax.dot_general(act, dy_blk, tn, preferred_element_type=F32)
        d2_copy(i).start()

        @pl.when(i + done0 < n_turn)
        def _():
            relay(0, i + done0)

        @pl.when(i + done0 >= n_turn)
        def _():
            relay(1, i + done0 - n_turn)

        return carry

    lax.fori_loop(0, 2 * n_tile, weight_step, 0)
    d2_copy(2 * n_tile - 1).wait()
    done1 = 2 * n_tile + done0 - n_turn
    for c in dy_loads:
        c.wait()
    lane = lax.broadcasted_iota(jnp.int32, (tokens, 128), 1)
    for m in range(n_micro):
        def gate_grad(j, total, m=m):
            i = m * top_k + j

            @pl.when(i + 1 < n_micro * top_k)
            def _():
                y_copy(i + 1).start()

            y_copy(i).wait()
            part = jnp.zeros((tokens, 128), F32)
            for c in range(0, d_model, 128):
                dy_blk = w2[0, (2 + m) * tokens:(3 + m) * tokens, c:c + 128].astype(F32)
                part = part + dy_blk * w2[0, pl.ds(pl.multiple_of((i % 2) * tokens, tokens), tokens), c:c + 128].astype(F32)
            @pl.when(i + done1 < n_turn - 2)
            def _():
                relay(1, i + done1)

            return jnp.where(lane == j, jnp.sum(part, axis=1, keepdims=True), total)

        total = lax.fori_loop(0, top_k, gate_grad, jnp.zeros((tokens, 128), F32))
        dg_ref[:, m, :] = jnp.transpose(total)[0:top_k, :]
    combine(0)
    relays(1, n_turn - 2, n_turn)
    combine(1)
    pltpu.make_async_copy(sent_part(1), sent_part(1), full_send.at[1]).wait()
    n_leaf = sum(len(set(p)) for p in LEAVES)
    part = leaf.at[:, :, pl.ds(0, n_leaf // 2)]
    pltpu.make_async_copy(part, part, leaf_send).wait()
    pltpu.make_async_copy(sib, sib, sib_send).wait()
    pltpu.make_async_copy(route.at[pl.ds(0, n_route)], route.at[pl.ds(0, n_route)], route_send).wait()
    for m in range(n_micro):
        pltpu.make_async_copy(ret.at[m, pl.ds(0, n_home)], ret.at[m, pl.ds(0, n_home)], ret_send.at[m]).wait()
        pltpu.make_async_copy(land.at[m], land.at[m], turn_send.at[m]).wait()


def solution(mesh):
    n_dev = mesh.shape['ep']
    side = 1
    while 2 * side * side < n_dev:
        side += 1
    tok_spec = P(None, ('dp', 'ep'))
    w_spec = P('ep')
    grad_w_spec = P(('dp', 'ep'))

    def local_step(grad_out, expert_out, gate_vals, topk_idx, slot_idx, x_dispatch, h1_pre, h3_pre, w_gate, w_up, w_down):
        n_micro, tokens, top_k, d_model = expert_out.shape
        local_exp, _, d_ff = w_gate.shape
        rows = x_dispatch.shape[2]
        capacity = rows // n_dev
        half = d_model // 2
        hbm = pl.BlockSpec(memory_space=pl.ANY)
        by_choice = functools.partial(jnp.transpose, axes=(2, 0, 1))
        vmem = pl.BlockSpec(memory_space=pltpu.VMEM)
        dma = pltpu.SemaphoreType.DMA
        kernel = functools.partial(exchange_kernel, n_dev, side, n_micro, tokens, top_k, d_model, d_ff, capacity)
        ff_shape = (n_micro, local_exp, rows, d_ff)
        wide_shape = (n_micro, local_exp, rows, d_model)
        out_vmem = pltpu.VMEM
        grad_x, grad_gate, grad_w_gate, grad_w_up, grad_w_down = pl.pallas_call(
            kernel,
            name='exchange',
            out_shape=(
                out_vmem((n_micro, tokens, d_model), BF16),
                out_vmem((top_k, n_micro, tokens), F32),
                out_vmem(w_gate.shape, F32),
                out_vmem(w_up.shape, F32),
                pltpu.HBM(w_down.shape, F32),
            ),
            in_specs=[hbm, hbm, vmem, vmem, vmem, hbm, hbm, hbm, hbm, hbm, hbm],
            out_specs=(vmem,) * 4 + (hbm,),
            scratch_shapes=[
                pltpu.VMEM((n_micro, 2, 2, 4, tokens, half), BF16),
                pltpu.VMEM((n_micro, 2, len(NODES), 2, 2, local_exp, capacity, half), BF16),
                pltpu.VMEM((n_micro, 2, len(NODES), local_exp, capacity, half), BF16),
                pltpu.VMEM(wide_shape, BF16),
                pltpu.VMEM((2, local_exp, rows // tokens, tokens, half), BF16),
                pltpu.VMEM((n_micro, n_dev, 2, local_exp, capacity, half), BF16),
                pltpu.VMEM((n_micro, side * (side - 1), 2, local_exp, 2 * capacity, half), BF16),
                pltpu.VMEM((1, d_ff, d_ff // 2), F32),
                pltpu.VMEM((n_dev, n_micro, 16, tokens), F32),
                pltpu.VMEM((tokens, 128), F32),
                pltpu.VMEM(w_gate.shape, BF16),
                pltpu.VMEM(w_up.shape, BF16),
                pltpu.VMEM(w_down.shape, BF16),
                pltpu.VMEM(ff_shape, BF16),
                pltpu.VMEM(ff_shape, BF16),
                pltpu.VMEM(ff_shape, BF16),
                pltpu.VMEM((tokens, n_dev * local_exp * capacity), BF16),
                dma((n_micro, 2, 8)),
                dma((n_micro,)),
                dma, dma,
                dma((n_micro,)),
                dma, dma,
                dma((n_micro,)),
                dma((n_micro,)),
                dma((n_micro,)),
                dma((n_micro, side * (side - 1))),
                dma((5,)),
                dma((2,)),
                dma((2, n_micro)),
                dma((2,)),
            ],
            compiler_params=pltpu.CompilerParams(collective_id=0, has_side_effects=True, vmem_limit_bytes=VMEM_GRANT),
            cost_estimate=pl.CostEstimate(flops=10 ** 10, bytes_accessed=5 * 10 ** 7, transcendentals=0),
        )(grad_out, jnp.transpose(expert_out, (0, 2, 1, 3)), by_choice(gate_vals), by_choice(topk_idx), by_choice(slot_idx),
          x_dispatch, h1_pre, h3_pre, w_gate, w_up, w_down)
        grad_gate = jnp.transpose(grad_gate, (1, 2, 0))
        return grad_x, grad_gate, grad_w_gate, grad_w_up, grad_w_down

    in_specs = (tok_spec,) * 8 + (w_spec,) * 3
    out_specs = (tok_spec, tok_spec, grad_w_spec, grad_w_spec, grad_w_spec)
    return jax.shard_map(local_step, mesh=mesh, in_specs=in_specs, out_specs=out_specs, check_vma=False)
```

```python
import functools
import jax
import jax.numpy as jnp
from jax import lax
from jax.experimental import pallas as pl
from jax.experimental.pallas import tpu as pltpu
from jax.sharding import PartitionSpec as P

MESH = pl.DeviceIdType.MESH
BF16 = jnp.bfloat16
VMEM_GRANT = 67043328 - 13 * 2 ** 20 + 160 * 2 ** 10
F32 = jnp.float32
NODES = ((0, 0), (1, 0), (0, 1), (2, 0), (0, 2), (2, 3))
EDGES = ((0, (1, 0), 1), (0, (0, 1), 2), (1, (1, 0), 3), (2, (0, 1), 4), (3, (0, -1), 5))
LEAVES = (((-1, 0), (0, -1)), ((0, 1), (0, -1)), ((-1, 0), (-1, 0)), ((0, 1), (0, 1)), ((1, 0), (-1, 0)), ((0, -1), (1, 0)))


def exchange_kernel(n_dev, side, n_micro, tokens, top_k, d_model, d_ff, capacity,
                    dy_hbm, yd_hbm, gate_ref, topk_ref, slot_ref, x_hbm, h1_hbm, h3_hbm, w1_hbm, w3_hbm, w2_hbm,
                    dx_ref, dg_ref, dw1_ref, dw3_ref, dw2_hbm,
                    full, leaf, sib, dyd, dxs, ret, land, d2, route, pad, w1, w3, w2, h1, h3, act_v, onehot,
                    full_recv, full_send, leaf_send, sib_send, dyd_recv, route_send, route_recv,
                    ret_send, ret_recv, turn_send, turn_recv, load_sem, y_sem, x_sem, d2_sem):
    me = lax.axis_index('ep')
    core = me % 2
    chip_x = (me // 2) % side
    chip_y = me // (2 * side)
    rows_dev = 2 * capacity
    half = d_model // 2

    def device(da, db, which):
        dx = da * (1 - core) + db * core
        dy = da * core + db * (1 - core)
        return (((chip_y + dy + 2 * side) % side) * side + (chip_x + dx + 2 * side) % side) * 2 + which

    def load_own(m, h):
        return pltpu.make_async_copy(dy_hbm.at[m, :, pl.ds(h * half, half)], full.at[m, h, 0, 0], full_recv.at[m, h, 0])

    for m in range(n_micro):
        for h in range(2):
            load_own(m, h).start()
    loads = [pltpu.make_async_copy(src, dst, load_sem.at[i]) for i, (src, dst) in enumerate(
        ((w2_hbm, w2), (h1_hbm, h1), (h3_hbm, h3), (w1_hbm, w1), (w3_hbm, w3)))]

    barrier = pltpu.get_barrier_semaphore()

    def greet(k, carry):
        pl.semaphore_signal(barrier, inc=1, device_id={'ep': (me + k) % n_dev}, device_id_type=MESH)
        return carry

    lax.fori_loop(1, n_dev, greet, 0)
    for c in loads:
        c.start()

    for m in range(n_micro):
        slot = slot_ref[:, m, :]
        key = jnp.where(slot >= 0, topk_ref[:, m, :] * capacity + slot, -1)
        route[me, m] = jnp.zeros((16, tokens), F32)
        route[me, m, 0:top_k] = key.astype(F32)
        route[me, m, 8:8 + top_k] = gate_ref[:, m, :]
    pl.semaphore_wait(barrier, n_dev - 1)

    def send_route(da, db):
        pltpu.make_async_remote_copy(route.at[me], route.at[me], route_send, route_recv,
                                     device_id={'ep': device(da, db, core)}, device_id_type=MESH).start()

    n_route = 0
    for da, db in sorted({(q * a % side, q * b % side) for a, b in NODES[1:] for q in (1, -1)}):
        send_route(da, db)
        n_route += 1

    def send_full(m, h, ev, da, db, slot):
        pltpu.make_async_remote_copy(full.at[m, h, ev // 4, ev % 4], full.at[m, h, slot // 4, slot % 4],
                                     full_send.at[m], full_recv.at[m, h, slot],
                                     device_id={'ep': device(da, db, core)}, device_id_type=MESH).start()

    def forward(m, h, ev):
        s = 1 - 2 * h
        tok = full.at[m, h, ev // 4, ev % 4]
        pltpu.make_async_copy(tok, tok, full_recv.at[m, h, ev]).wait()
        for src, (da, db), slot in EDGES:
            @pl.when(ev == src)
            def _(da=da, db=db, slot=slot):
                send_full(m, h, ev, s * da, s * db, slot)

    def by_event(ev, values):
        out = values[0]
        for i, v in enumerate(values[1:]):
            out = jnp.where(ev == i + 1, v, out)
        return out

    def pack(m, h, ev):
        s = 1 - 2 * h
        tok = full.at[m, h, ev // 4, ev % 4]
        home = device(-s * by_event(ev, [p[0] for p in NODES]), -s * by_event(ev, [p[1] for p in NODES]), core)
        leaf_chip = [device(s * by_event(ev, [p[i][0] for p in LEAVES]), s * by_event(ev, [p[i][1] for p in LEAVES]), 0)
                     for i in range(2)]
        row = lax.broadcasted_iota(jnp.int32, (6 * rows_dev, tokens), 0)
        block = row // rows_dev
        inner = row - block * rows_dev
        dev = jnp.where(block < 4, leaf_chip[0] + block - 2, leaf_chip[1] + block - 4)
        dev = jnp.where(block == 0, me, jnp.where(block == 1, me + 1 - 2 * core, dev))
        want = (dev * rows_dev + inner).astype(F32)
        table = route[home, m]
        pick = jnp.zeros((6 * rows_dev, tokens), F32)
        gate = jnp.zeros((6 * rows_dev, tokens), F32)
        for j in range(top_k):
            hit = want == table[j:j + 1, :]
            pick = jnp.where(hit, 1.0, pick)
            gate = jnp.where(hit, table[8 + j:9 + j, :], gate)
        gate = jnp.sum(gate, axis=1, keepdims=True)
        rows = jnp.dot(pick.astype(BF16), tok[...], preferred_element_type=F32)
        rows = (rows * gate).astype(BF16)
        leaf[m, h, ev] = rows[2 * rows_dev:].reshape(2, 2, 2, capacity, half)
        sib[m, h, ev] = rows[rows_dev:2 * rows_dev].reshape(2, capacity, half)
        row0 = pl.multiple_of(home * capacity, capacity)
        col0 = pl.multiple_of(h * half, half)
        dyd[m, :, pl.ds(row0, capacity), pl.ds(col0, half)] = rows[:rows_dev].reshape(2, capacity, half)
        target = dyd.at[m, :, pl.ds(row0, capacity), pl.ds(col0, half)]

        def send_leaf(i):
            for c in range(2):
                pltpu.make_async_remote_copy(leaf.at[m, h, ev, i, c], target, leaf_send, dyd_recv.at[m],
                                             device_id={'ep': leaf_chip[i] + c}, device_id_type=MESH).start()

        send_leaf(0)

        @pl.when(by_event(ev, [int(len(set(p)) == 2) for p in LEAVES]) == 1)
        def _():
            send_leaf(1)

        pltpu.make_async_remote_copy(sib.at[m, h, ev], target, sib_send, dyd_recv.at[m],
                                     device_id={'ep': me + 1 - 2 * core}, device_id_type=MESH).start()

    def item(m, ev):
        for h in range(2):
            forward(m, h, ev)
        for h in range(2):
            pack(m, h, ev)

    def items(m, lo, hi):
        lax.fori_loop(lo, hi, lambda ev, c: (item(m, ev), c)[1], 0)

    chunk = 256
    per_exp = (n_dev * capacity) // chunk

    def out_rows(m):
        return dxs if m == 0 else full.at[0]

    def own_rows(m, dst):
        row0 = pl.multiple_of((dst % (tokens // capacity)) * capacity, capacity)
        return out_rows(m).at[:, :, dst // (tokens // capacity), pl.ds(row0, capacity), :]

    def compute(m, c):
        e = c // per_exp
        r0 = pl.multiple_of((c % per_exp) * chunk, chunk)
        nt = (((1,), (1,)), ((), ()))
        grad_act = lax.dot_general(dyd[m, e, pl.ds(r0, chunk)], w2[e], nt, preferred_element_type=F32)
        grad_act = grad_act.astype(BF16).astype(F32)
        h1_f32 = h1[m, e, pl.ds(r0, chunk)].astype(F32)
        h3_f32 = h3[m, e, pl.ds(r0, chunk)].astype(F32)
        sig = jax.nn.sigmoid(h1_f32)
        silu = h1_f32 * sig
        act = (silu * h3_f32).astype(BF16)
        grad_h1 = (grad_act * h3_f32 * sig * (1.0 + h1_f32 * (1.0 - sig))).astype(BF16)
        grad_h3 = (grad_act * silu).astype(BF16)
        rows = lax.dot_general(grad_h1, w1[e], nt, preferred_element_type=F32)
        rows = rows + lax.dot_general(grad_h3, w3[e], nt, preferred_element_type=F32)
        rows = rows.astype(BF16)
        blk = (c % per_exp) * (chunk // tokens)
        for h in range(2):
            out_rows(m)[h, e, pl.ds(blk, chunk // tokens)] = rows[:, h * half:(h + 1) * half].reshape(-1, tokens, half)
        h1[m, e, pl.ds(r0, chunk)] = grad_h1
        h3[m, e, pl.ds(r0, chunk)] = grad_h3
        act_v[m, e, pl.ds(r0, chunk)] = act

    pair_rows = 2 * capacity
    n_turn = side * (side - 1)

    def send_home(src, m, owner, dst):
        pltpu.make_async_remote_copy(src, ret.at[m, owner], ret_send.at[m], ret_recv.at[m],
                                     device_id={'ep': dst}, device_id_type=MESH).start()

    def send_return(m):
        def turn(i, carry):
            da, db = (i // (side - 1) + 1) % side, i % (side - 1) + 1
            chip = device(da, db, 0) // 2
            per_blk = tokens // pair_rows
            row0 = pl.multiple_of((chip % per_blk) * pair_rows, pair_rows)
            pltpu.make_async_remote_copy(out_rows(m).at[:, :, chip // per_blk, pl.ds(row0, pair_rows), :], land.at[m, i],
                                         turn_send.at[m], turn_recv.at[m, i],
                                         device_id={'ep': device(0, db, core)}, device_id_type=MESH).start()
            return carry

        def straight(i, carry):
            dst = device(i // 2, 0, i % 2)
            send_home(own_rows(m, dst), m, me, dst)
            return carry

        lax.fori_loop(2, 2 * side, straight, 0)
        lax.fori_loop(0, n_turn, turn, 0)
        send_home(own_rows(m, me + 1 - 2 * core), m, me, me + 1 - 2 * core)

    def relay(m, i):
        da, db = (i // (side - 1) + 1) % side, i % (side - 1) + 1
        pltpu.make_async_copy(land.at[m, i], land.at[m, i], turn_recv.at[m, i]).wait()
        owner = device(0, -db, core)

        def part(which):
            return land.at[m, i, :, :, pl.ds(pl.multiple_of(which * capacity, capacity), capacity), :]

        @pl.when(da != 0)
        def _():
            for which in range(2):
                send_home(part(which), m, owner, device(da, 0, which))

        @pl.when(da == 0)
        def _():
            send_home(part(1 - core), m, owner, me + 1 - 2 * core)
            ret[m, owner] = part(core)[...]

    def relays(m, lo, hi):
        lax.fori_loop(lo, hi, lambda i, c: (relay(m, i), c)[1], 0)

    n_home = n_dev - side

    def combine(m):
        pad[...] = jnp.zeros_like(pad)
        pad[0:16] = route[me, m]
        key = jnp.transpose(pad[...])
        place = lax.broadcasted_iota(jnp.int32, (tokens, n_dev * rows_dev), 1).astype(F32)
        mat = jnp.zeros((tokens, n_dev * rows_dev), F32)
        for j in range(top_k):
            mat = jnp.where(place == key[:, j:j + 1], 1.0, mat)
        onehot[...] = mat.astype(BF16)
        ret[m, me] = own_rows(m, me)[...]
        pltpu.make_async_copy(ret.at[m, pl.ds(0, n_home)], ret.at[m, pl.ds(0, n_home)], ret_recv.at[m]).wait()
        for h in range(2):
            for c in range(0, half, 256):
                back = ret[m, :, h, :, :, c:c + 256].reshape(n_dev * rows_dev, 256)
                dx_ref[m, :, h * half + c:h * half + c + 256] = jnp.dot(
                    onehot[...], back, preferred_element_type=F32).astype(BF16)

    pltpu.make_async_copy(route.at[pl.ds(0, n_route)], route.at[pl.ds(0, n_route)], route_recv).wait()
    items(0, 0, 1)
    items(1, 0, 1)
    items(0, 1, 6)
    items(1, 1, 2)

    def sent_part(m):
        return full.at[m, :, :, :, pl.ds(0, len(EDGES) * tokens // 8), :]

    def wait_dyd(m):
        part = dyd.at[m, :, pl.ds(0, (n_dev - len(NODES)) * capacity)]
        pltpu.make_async_copy(part, part, dyd_recv.at[m]).wait()

    for c in loads:
        c.wait()
    wait_dyd(0)

    def mixed(c, carry):
        compute(0, c)
        item(1, 2 + c)
        return carry

    lax.fori_loop(0, 2 * per_exp, mixed, 0)
    send_return(0)
    wait_dyd(1)
    pltpu.make_async_copy(sent_part(0), sent_part(0), full_send.at[0]).wait()
    lax.fori_loop(0, 2 * per_exp, lambda c, carry: (compute(1, c), carry)[1], 0)
    send_return(1)

    tile = d_ff // 2
    n_tile = d_model // tile
    rows_exp = n_dev * capacity

    def x_copy(i, m):
        col = pl.multiple_of((i % n_tile) * tile, tile)
        return pltpu.make_async_copy(x_hbm.at[m, i // n_tile, :, pl.ds(col, tile)],
                                     w1.at[i % 2, pl.ds(m * rows_exp, rows_exp), pl.ds(0, tile)], x_sem.at[i % 2, m])

    def dy_block(m):
        return w2.at[0, pl.ds((2 + m) * tokens, tokens), :]

    def y_copy(i):
        return pltpu.make_async_copy(yd_hbm.at[i // top_k, i % top_k],
                                     w2.at[0, pl.ds(pl.multiple_of((i % 2) * tokens, tokens), tokens), :], y_sem.at[i % 2])

    dy_loads = [pltpu.make_async_copy(dy_hbm.at[m], dy_block(m), load_sem.at[m]) for m in range(n_micro)]
    for m in range(n_micro):
        x_copy(0, m).start()
        dy_loads[m].start()
    y_copy(0).start()

    done0 = 0

    def d2_copy(i):
        col = pl.multiple_of((i % n_tile) * tile, tile)
        return pltpu.make_async_copy(d2.at[0], dw2_hbm.at[i // n_tile, :, pl.ds(col, tile)], d2_sem.at[0])

    def weight_step(i, carry):
        @pl.when(i + 1 < 2 * n_tile)
        def _():
            for m in range(n_micro):
                x_copy(i + 1, m).start()

        for m in range(n_micro):
            x_copy(i, m).wait()
        e = i // n_tile
        col = pl.multiple_of((i % n_tile) * tile, tile)
        tn = (((0,), (0,)), ((), ()))
        x_blk = w1[i % 2, 0:n_micro * rows_exp, 0:tile]
        g1 = h1[:, e].reshape(n_micro * rows_exp, d_ff)
        g3 = h3[:, e].reshape(n_micro * rows_exp, d_ff)
        act = act_v[:, e].reshape(n_micro * rows_exp, d_ff)
        dy_blk = dyd[:, e, :, pl.ds(col, tile)].reshape(n_micro * rows_exp, tile)
        dw1_ref[e, pl.ds(col, tile), :] = lax.dot_general(x_blk, g1, tn, preferred_element_type=F32)
        dw3_ref[e, pl.ds(col, tile), :] = lax.dot_general(x_blk, g3, tn, preferred_element_type=F32)
        @pl.when(i >= 1)
        def _():
            d2_copy(i - 1).wait()

        d2[0] = lax.dot_general(act, dy_blk, tn, preferred_element_type=F32)
        d2_copy(i).start()

        @pl.when(i + done0 < n_turn)
        def _():
            relay(0, i + done0)

        @pl.when(i + done0 >= n_turn)
        def _():
            relay(1, i + done0 - n_turn)

        return carry

    lax.fori_loop(0, 2 * n_tile, weight_step, 0)
    d2_copy(2 * n_tile - 1).wait()
    done1 = 2 * n_tile + done0 - n_turn
    for c in dy_loads:
        c.wait()
    lane = lax.broadcasted_iota(jnp.int32, (tokens, 128), 1)
    for m in range(n_micro):
        def gate_grad(j, total, m=m):
            i = m * top_k + j

            @pl.when(i + 1 < n_micro * top_k)
            def _():
                y_copy(i + 1).start()

            y_copy(i).wait()
            part = jnp.zeros((tokens, 128), F32)
            for c in range(0, d_model, 128):
                dy_blk = w2[0, (2 + m) * tokens:(3 + m) * tokens, c:c + 128].astype(F32)
                part = part + dy_blk * w2[0, pl.ds(pl.multiple_of((i % 2) * tokens, tokens), tokens), c:c + 128].astype(F32)
            @pl.when(i + done1 < n_turn - 2)
            def _():
                relay(1, i + done1)

            return jnp.where(lane == j, jnp.sum(part, axis=1, keepdims=True), total)

        total = lax.fori_loop(0, top_k, gate_grad, jnp.zeros((tokens, 128), F32))
        dg_ref[:, m, :] = jnp.transpose(total)[0:top_k, :]
    combine(0)
    relays(1, n_turn - 2, n_turn)
    combine(1)
    pltpu.make_async_copy(sent_part(1), sent_part(1), full_send.at[1]).wait()
    n_leaf = sum(len(set(p)) for p in LEAVES)
    part = leaf.at[:, :, pl.ds(0, n_leaf // 2)]
    pltpu.make_async_copy(part, part, leaf_send).wait()
    pltpu.make_async_copy(sib, sib, sib_send).wait()
    pltpu.make_async_copy(route.at[pl.ds(0, n_route)], route.at[pl.ds(0, n_route)], route_send).wait()
    for m in range(n_micro):
        pltpu.make_async_copy(ret.at[m, pl.ds(0, n_home)], ret.at[m, pl.ds(0, n_home)], ret_send.at[m]).wait()
        pltpu.make_async_copy(land.at[m], land.at[m], turn_send.at[m]).wait()


def finish_kernel(dx_ref, dg_ref, dw1_ref, dw3_ref, dx_out, dg_out, dw1_out, dw3_out, sem):
    copies = [pltpu.make_async_copy(src, dst, sem.at[i]) for i, (src, dst) in enumerate(
        ((dw1_ref, dw1_out), (dw3_ref, dw3_out), (dx_ref, dx_out), (dg_ref, dg_out)))]
    for c in copies:
        c.start()
    for c in copies:
        c.wait()


def finish(results):
    return pl.pallas_call(
        finish_kernel,
        name='finish',
        out_shape=tuple(jax.ShapeDtypeStruct(r.shape, r.dtype) for r in results),
        in_specs=[pl.BlockSpec(memory_space=pltpu.VMEM)] * 4,
        out_specs=(pl.BlockSpec(memory_space=pl.ANY),) * 4,
        scratch_shapes=[pltpu.SemaphoreType.DMA((4,))],
        compiler_params=pltpu.CompilerParams(vmem_limit_bytes=2 ** 20),
    )(*results)


def solution(mesh):
    n_dev = mesh.shape['ep']
    side = 1
    while 2 * side * side < n_dev:
        side += 1
    tok_spec = P(None, ('dp', 'ep'))
    w_spec = P('ep')
    grad_w_spec = P(('dp', 'ep'))

    def local_step(grad_out, expert_out, gate_vals, topk_idx, slot_idx, x_dispatch, h1_pre, h3_pre, w_gate, w_up, w_down):
        n_micro, tokens, top_k, d_model = expert_out.shape
        local_exp, _, d_ff = w_gate.shape
        rows = x_dispatch.shape[2]
        capacity = rows // n_dev
        half = d_model // 2
        hbm = pl.BlockSpec(memory_space=pl.ANY)
        by_choice = functools.partial(jnp.transpose, axes=(2, 0, 1))
        vmem = pl.BlockSpec(memory_space=pltpu.VMEM)
        dma = pltpu.SemaphoreType.DMA
        kernel = functools.partial(exchange_kernel, n_dev, side, n_micro, tokens, top_k, d_model, d_ff, capacity)
        ff_shape = (n_micro, local_exp, rows, d_ff)
        wide_shape = (n_micro, local_exp, rows, d_model)
        out_vmem = pltpu.VMEM
        *results, grad_w_down = pl.pallas_call(
            kernel,
            name='exchange',
            out_shape=(
                out_vmem((n_micro, tokens, d_model), BF16),
                out_vmem((top_k, n_micro, tokens), F32),
                out_vmem(w_gate.shape, F32),
                out_vmem(w_up.shape, F32),
                pltpu.HBM(w_down.shape, F32),
            ),
            in_specs=[hbm, hbm, vmem, vmem, vmem, hbm, hbm, hbm, hbm, hbm, hbm],
            out_specs=(vmem,) * 4 + (hbm,),
            scratch_shapes=[
                pltpu.VMEM((n_micro, 2, 2, 4, tokens, half), BF16),
                pltpu.VMEM((n_micro, 2, len(NODES), 2, 2, local_exp, capacity, half), BF16),
                pltpu.VMEM((n_micro, 2, len(NODES), local_exp, capacity, half), BF16),
                pltpu.VMEM(wide_shape, BF16),
                pltpu.VMEM((2, local_exp, rows // tokens, tokens, half), BF16),
                pltpu.VMEM((n_micro, n_dev, 2, local_exp, capacity, half), BF16),
                pltpu.VMEM((n_micro, side * (side - 1), 2, local_exp, 2 * capacity, half), BF16),
                pltpu.VMEM((1, d_ff, d_ff // 2), F32),
                pltpu.VMEM((n_dev, n_micro, 16, tokens), F32),
                pltpu.VMEM((tokens, 128), F32),
                pltpu.VMEM(w_gate.shape, BF16),
                pltpu.VMEM(w_up.shape, BF16),
                pltpu.VMEM(w_down.shape, BF16),
                pltpu.VMEM(ff_shape, BF16),
                pltpu.VMEM(ff_shape, BF16),
                pltpu.VMEM(ff_shape, BF16),
                pltpu.VMEM((tokens, n_dev * local_exp * capacity), BF16),
                dma((n_micro, 2, 8)),
                dma((n_micro,)),
                dma, dma,
                dma((n_micro,)),
                dma, dma,
                dma((n_micro,)),
                dma((n_micro,)),
                dma((n_micro,)),
                dma((n_micro, side * (side - 1))),
                dma((5,)),
                dma((2,)),
                dma((2, n_micro)),
                dma((2,)),
            ],
            compiler_params=pltpu.CompilerParams(collective_id=0, has_side_effects=True, vmem_limit_bytes=VMEM_GRANT),
            cost_estimate=pl.CostEstimate(flops=10 ** 10, bytes_accessed=5 * 10 ** 7, transcendentals=0),
        )(grad_out, jnp.transpose(expert_out, (0, 2, 1, 3)), by_choice(gate_vals), by_choice(topk_idx), by_choice(slot_idx),
          x_dispatch, h1_pre, h3_pre, w_gate, w_up, w_down)
        grad_x, grad_gate, grad_w_gate, grad_w_up = finish(results)
        grad_gate = jnp.transpose(grad_gate, (1, 2, 0))
        return grad_x, grad_gate, grad_w_gate, grad_w_up, grad_w_down

    in_specs = (tok_spec,) * 8 + (w_spec,) * 3
    out_specs = (tok_spec, tok_spec, grad_w_spec, grad_w_spec, grad_w_spec)
    return jax.shard_map(local_step, mesh=mesh, in_specs=in_specs, out_specs=out_specs, check_vma=False)
```
